32 devices in a mesh: mode: 8 (over y, x, core), tm: 4 (over z).
Axes of the slice: x: 2, y: 2, z: 4, core: 2. Of those that a mesh axis runs over, the one named last changes fastest.
Arguments:
- field: float32 [2, 128, 65536], P(None, 'mode', 'tm'), may hold values from -1.8 to 1.8
- beta: float32 [3, 128], P(None, 'mode'), may hold values from -1 to 1
- quartets: int32 [4, 1024], replicated, may hold values from 0 to 127
- intersections: float32 [1024], replicated, may hold values from -0.12 to 0.12
Outputs:
- field_out: float32 [2, 128, 65536], P(None, 'mode', 'tm')
- errors: float32 [2, 128], P(None, 'mode')
The draws below stay inside these ranges and needn't reach their ends.
All inputs are finite; a program needn't handle non-finite values.
Results may differ from the reference program's by a relative error of at most 0.0003.
Values sent between devices are 32-bit elements; how exact they have to be, the bound alone decides.
A program may use at most 128 MiB of HBM per device.

```python
import math
import jax
import jax.numpy as jnp
from jax import lax

MODES = 128
TIME = 65536
STEPS = 2
QUARTETS = 1024


def draw_field(key, part):
    first_key = jax.random.fold_in(key, 0)
    ramp = lax.iota(jnp.float32, TIME) / TIME
    envelope = 0.6 * (1.0 + 2.0 * ramp)
    values = jnp.clip(0.5 * jax.random.normal(first_key, (2, MODES, TIME), jnp.float32), -1.0, 1.0)
    return (values * envelope).astype(jnp.float32)


def set_ends(array, key, low, top_value):
    shape = array.shape
    index_at = [jax.random.randint(jax.random.fold_in(key, axis), (), 0, shape[axis]) for axis in range(len(shape))]
    array = array.at[tuple(index_at)].set(low)
    longest = shape.index(max(shape))
    index_at[longest] = (index_at[longest] + 1) % shape[longest]
    return array.at[tuple(index_at)].set(top_value)


def block_levels(own_key, extent, cuts, low, largest):
    def one(position, shards_of):
        heights = jax.random.uniform(jax.random.fold_in(jax.random.fold_in(own_key, 6), position), (shards_of,), jnp.float32, low / len(cuts), largest / len(cuts))
        return jnp.repeat(jnp.exp(heights), extent[position] // shards_of).reshape((-1,) + (1,) * (len(extent) - position - 1))

    factor_of = one(*cuts[0])
    for cut in cuts[1:]:
        factor_of = factor_of * one(*cut)
    return factor_of


def bell_draw(rng, dims, scale, reach, dtype=jnp.bfloat16):
    return jnp.clip(scale * jax.random.normal(rng, dims, jnp.float32), -reach, reach).astype(dtype)


def setup_inputs(seed: int = 0) -> dict:
    seeds = jax.random.split(jax.random.key(seed), 5)
    return {
        "field": draw_field(jax.random.fold_in(seeds[4], 71), 0),
        "beta": jnp.clip(jax.random.uniform(seeds[1], (3, MODES), jnp.float32, -1.0, 1.0) * block_levels(seeds[1], (3, MODES), ((1, 8),), -0.4, 0.0), -1.0, 1.0),
        "quartets": set_ends(jax.random.randint(seeds[2], (4, QUARTETS), 0, MODES), jax.random.fold_in(seeds[2], 1), 0, MODES - 1).astype(jnp.int32),
        "intersections": bell_draw(seeds[3], (QUARTETS,), 0.03, 0.12, jnp.float32),
    }


epsilon = 1e-06

def phase_of(offset, slope, curve, frequency):
    return math.pi * offset + 300.0 * slope * frequency + 3000.0 * curve * frequency * frequency

def triple_product(left_field, middle_field, conj_field):
    prod_re = left_field[0] * middle_field[0] - left_field[1] * middle_field[1]
    prod_im = left_field[0] * middle_field[1] + left_field[1] * middle_field[0]
    out_re = prod_re * conj_field[0] + prod_im * conj_field[1]
    out_im = prod_im * conj_field[0] - prod_re * conj_field[1]
    return (out_re, out_im)

def kerr_term(fields, quartets, intersections):
    blocks = quartets.shape[1] // 128
    grouped = quartets.reshape(4, blocks, 128).transpose(1, 0, 2)
    weights = intersections.reshape(blocks, 128)

    def accumulate(running, block_item):
        indices, weight = block_item
        out_re, out_im = triple_product(fields[:, indices[1], :], fields[:, indices[2], :], fields[:, indices[3], :])
        contrib = jnp.stack([weight[:, None] * -out_im, weight[:, None] * out_re])
        return (running.at[:, indices[0], :].add(contrib), None)
    running, unused = lax.scan(accumulate, jnp.zeros_like(fields), (grouped, weights))
    return running

def reference(field, beta, quartets, intersections):
    sample_index = lax.iota(jnp.int32, TIME)
    signed = jnp.where(sample_index < TIME // 2, sample_index, sample_index - TIME)
    frequency = signed.astype(jnp.float32) / (TIME / 2)
    angle = phase_of(beta[0][:, None], beta[1][:, None], beta[2][:, None], frequency[None, :])
    rotor = lax.complex(jnp.cos(angle), jnp.sin(angle))
    error_rows = []
    for step_index in range(STEPS):
        spectrum = jnp.fft.fft(lax.complex(field[0], field[1]), axis=-1) * rotor
        moved = jnp.fft.ifft(spectrum, axis=-1)
        linear = jnp.stack([jnp.real(moved), jnp.imag(moved)])
        first = kerr_term(linear, quartets, intersections)
        second = kerr_term(linear + first, quartets, intersections)
        field = linear + 0.5 * (first + second)
        estimate = 0.5 * (second - first)
        error_sq = lax.optimization_barrier(jnp.sum(estimate * estimate, axis=(0, 2)))
        field_sq = lax.optimization_barrier(jnp.sum(field * field, axis=(0, 2)))
        error_rows.append(jnp.sqrt(error_sq / (field_sq + epsilon)))
    return (field, jnp.stack(error_rows))
```

```python
import functools
import math

import jax
import jax.numpy as jnp
from jax import lax
from jax.experimental import pallas as pl
from jax.experimental.pallas import tpu as pltpu
from jax.sharding import PartitionSpec as P

RADIX = 256
STEPS = 2


epsilon = 1e-06


def phase_of(offset, slope, curve, frequency):
    return math.pi * offset + 300.0 * slope * frequency + 3000.0 * curve * frequency * frequency


def triple_product(left_field, middle_field, conj_field):
    prod_re = left_field[0] * middle_field[0] - left_field[1] * middle_field[1]
    prod_im = left_field[0] * middle_field[1] + left_field[1] * middle_field[0]
    out_re = prod_re * conj_field[0] + prod_im * conj_field[1]
    out_im = prod_im * conj_field[0] - prod_re * conj_field[1]
    return (out_re, out_im)


def contract(form, first_operand, second_operand):
    return jnp.einsum(form, first_operand, second_operand, precision=lax.Precision.HIGHEST)


def rotate(real_part, imag_part, angle):
    cosine = jnp.cos(angle)
    sine_part = jnp.sin(angle)
    return (real_part * cosine - imag_part * sine_part, real_part * sine_part + imag_part * cosine)


def dft_tables(length):
    positions = lax.iota(jnp.int32, length)
    product = positions[:, None] * positions[None, :] % length
    angle = -2.0 * math.pi / length * product.astype(jnp.float32)
    return (jnp.cos(angle), jnp.sin(angle))


def to_columns(state):
    return lax.all_to_all(state, "tm", split_axis=3, concat_axis=2, tiled=True)


def to_rows(state):
    return lax.all_to_all(state, "tm", split_axis=2, concat_axis=3, tiled=True)


def linear_step(state, beta, table_re, table_im):
    radix_size = table_re.shape[0]
    total_time = radix_size * radix_size
    cols_local = state.shape[3]
    tm_index = lax.axis_index("tm")
    head_re = contract("ka,mab->mkb", table_re, state[0]) - contract(
        "ka,mab->mkb", table_im, state[1]
    )
    head_im = contract("ka,mab->mkb", table_re, state[1]) + contract(
        "ka,mab->mkb", table_im, state[0]
    )
    column = tm_index * cols_local + lax.iota(jnp.int32, cols_local)
    row_position = lax.iota(jnp.int32, radix_size)
    twist = (
        -2.0
        * math.pi
        / total_time
        * (row_position[:, None] * column[None, :] % total_time).astype(jnp.float32)
    )
    head_re, head_im = rotate(head_re, head_im, twist[None])
    turned = lax.all_to_all(
        jnp.stack([head_re, head_im]), "tm", split_axis=2, concat_axis=3, tiled=True
    )
    spec_re = contract("mcb,kb->mck", turned[0], table_re) - contract(
        "mcb,kb->mck", turned[1], table_im
    )
    spec_im = contract("mcb,kb->mck", turned[1], table_re) + contract(
        "mcb,kb->mck", turned[0], table_im
    )
    rows_local = turned.shape[2]
    first_index = tm_index * rows_local + lax.iota(jnp.int32, rows_local)
    wave = first_index[:, None] + radix_size * row_position[None, :]
    signed = jnp.where(wave < total_time // 2, wave, wave - total_time)
    frequency = signed.astype(jnp.float32) / (total_time / 2)
    angle = phase_of(
        beta[0][:, None, None], beta[1][:, None, None], beta[2][:, None, None], frequency[None]
    )
    spec_re, spec_im = rotate(spec_re, spec_im, angle)
    back_re = contract("mck,kb->mcb", spec_re, table_re) + contract(
        "mck,kb->mcb", spec_im, table_im
    )
    back_im = contract("mck,kb->mcb", spec_im, table_re) - contract(
        "mck,kb->mcb", spec_re, table_im
    )
    untwist = (
        2.0
        * math.pi
        / total_time
        * (first_index[:, None] * row_position[None, :] % total_time).astype(jnp.float32)
    )
    back_re, back_im = rotate(back_re, back_im, untwist[None])
    gathered = lax.all_to_all(
        jnp.stack([back_re, back_im]), "tm", split_axis=3, concat_axis=2, tiled=True
    )
    scale = 1.0 / total_time
    out_re = (
        contract("ka,mkb->mab", table_re, gathered[0])
        + contract("ka,mkb->mab", table_im, gathered[1])
    ) * scale
    out_im = (
        contract("ka,mkb->mab", table_re, gathered[1])
        - contract("ka,mkb->mab", table_im, gathered[0])
    ) * scale
    return jnp.stack([out_re, out_im])


def kerr_term(fields, quartets, intersections):
    count = quartets.shape[1]
    block_size = min(512, count)
    blocks = count // block_size
    grouped = quartets.reshape(4, blocks, block_size).transpose(1, 0, 2)
    weights = intersections.reshape(blocks, block_size)
    modes_all = fields.shape[1]
    mode_ids = lax.iota(jnp.int32, modes_all)

    def accumulate(running, block_item):
        indices, weight = block_item
        out_re, out_im = triple_product(
            jnp.take(fields, indices[1], axis=1),
            jnp.take(fields, indices[2], axis=1),
            jnp.take(fields, indices[3], axis=1),
        )
        owner = (indices[0][None, :] == mode_ids[:, None]).astype(jnp.float32) * weight[None, :]
        add_re = contract("pq,qt->pt", owner, -out_im)
        add_im = contract("pq,qt->pt", owner, out_re)
        return (running + jnp.stack([add_re, add_im]), None)

    running, unused = lax.scan(accumulate, jnp.zeros_like(fields), (grouped, weights))
    return running


def kerr_step(flat, quartets, intersections):
    spread = lax.all_to_all(flat, "mode", split_axis=2, concat_axis=1, tiled=True)
    first = kerr_term(spread, quartets, intersections)
    second = kerr_term(spread + first, quartets, intersections)
    updated = spread + 0.5 * (first + second)
    estimate = 0.5 * (second - first)
    returned, estimate_home = (
        lax.all_to_all(updated, "mode", split_axis=1, concat_axis=2, tiled=True),
        lax.all_to_all(estimate, "mode", split_axis=1, concat_axis=2, tiled=True),
    )
    error_part = jnp.sum(estimate_home * estimate_home, axis=(0, 2))
    field_part = jnp.sum(returned * returned, axis=(0, 2))
    return (returned, error_part, field_part)


def shards_general(field, beta, quartets, intersections):
    modes_local = field.shape[1]
    time_local = field.shape[2]
    table_re, table_im = dft_tables(RADIX)
    state = field.reshape(2, modes_local, time_local // RADIX, RADIX)
    state = to_columns(state)
    error_rows = []
    for step_index in range(STEPS):
        columns = state
        columns = linear_step(columns, beta, table_re, table_im)
        updated, error_part, field_part = kerr_step(
            columns.reshape(2, modes_local, time_local), quartets, intersections
        )
        error_sq, field_sq = lax.psum((error_part, field_part), "tm")
        error_rows.append(jnp.sqrt(error_sq / (field_sq + epsilon)))
        state = updated.reshape(columns.shape)
    state = to_rows(state)
    errors = jnp.stack(error_rows)
    return (state.reshape(2, modes_local, time_local), errors)


UNROLL = 8
MESH = pl.DeviceIdType.MESH


def split(value):
    high = value.astype(jnp.bfloat16)
    low = (value - high.astype(jnp.float32)).astype(jnp.bfloat16)
    return high, low


def split_table(value):
    high = lax.reduce_precision(value, exponent_bits=8, mantissa_bits=7)
    return high.astype(jnp.bfloat16), (value - high).astype(jnp.bfloat16)


def product(left, right):
    dot = lambda a, b: jnp.dot(a, b, preferred_element_type=jnp.float32)
    return dot(left[0], right[0]) + (dot(left[0], right[1]) + dot(left[1], right[0]))


def transform(real, imag, m1, m2, twist_ref, ro_re, ro_im):
    radix = twist_ref.shape[1]
    head = product(m1, split(jnp.concatenate([real, imag], axis=0)))
    head_re, head_im = head[:radix], head[radix:]
    tw_re, tw_im = twist_ref[0], twist_ref[1]
    re = head_re * tw_re - head_im * tw_im
    im = head_re * tw_im + head_im * tw_re
    spec = product(split(jnp.concatenate([re, im], axis=1)), m2)
    spec_re, spec_im = spec[:, :radix], spec[:, radix:]
    re = spec_re * ro_re - spec_im * ro_im
    im = spec_re * ro_im + spec_im * ro_re
    back = product(split(jnp.concatenate([re, im], axis=1)), m1)
    back_re, back_im = back[:, :radix], back[:, radix:]
    re = back_re * tw_re + back_im * tw_im
    im = back_im * tw_re - back_re * tw_im
    out = product(m2, split(jnp.concatenate([re, im], axis=0)))
    return out[:radix], out[radix:]


def step_kernel(
    ways, own, index_ref, last_ref, weight_ref, keep_ref, has_ref,
    x_ref, m1h, m1l, m2h, m2l, twist_ref, rotor_ref,
    out_ref, err_ref,
    sent, held_00, held_01, held_10, held_11, mid, first, partial, updated, back, final, sums, norm, norms,
    send_sems, recv_sems,
):
    mode_ways, tm_ways = ways
    devices = mode_ways * tm_ways
    planes = 2 * own
    held = ((held_00, held_01), (held_10, held_11))
    my_mode, my_tm = lax.axis_index("mode"), lax.axis_index("tm")
    me = my_tm * mode_ways + my_mode
    radix = twist_ref.shape[1]
    half = radix // 2
    count = weight_ref.shape[0]
    unroll = UNROLL if count % UNROLL == 0 else 1

    def partner(k):
        tm = lax.rem(my_tm + lax.rem(k, tm_ways), tm_ways)
        mode = lax.rem(my_mode + k // tm_ways, mode_ways)
        return mode, tm, tm * mode_ways + mode

    barrier = pltpu.get_barrier_semaphore()

    def greet(k, carry):
        mode, tm, _ = partner(k)
        pl.semaphore_signal(barrier, inc=1, device_id=(mode, tm), device_id_type=MESH)
        return carry

    lax.fori_loop(1, devices, greet, 0)

    def to_all(pick_src, dst, slot):
        def one(k, carry):
            mode, tm, holder = partner(k)
            pltpu.make_async_remote_copy(
                src_ref=pick_src(holder),
                dst_ref=dst,
                send_sem=send_sems.at[slot],
                recv_sem=recv_sems.at[slot],
                device_id=(mode, tm),
                device_id_type=MESH,
            ).start()
            return carry

        lax.fori_loop(1, devices, one, 0)

    def arrived(ref, slot):
        pltpu.make_async_copy(ref, ref, recv_sems.at[slot]).wait()

    def drained(ref, slot):
        pltpu.make_async_copy(ref, ref, send_sems.at[slot]).wait()

    def spectral(load, step, base):
        m1, m2 = (m1h[...], m1l[...]), (m2h[...], m2l[...])

        def one(g, carry):
            real, imag = load(g)
            re, im = transform(real, imag, m1, m2, twist_ref, rotor_ref[0, g], rotor_ref[1, g])
            for part, value in enumerate((re, im)):
                for h in range(2):
                    piece = value[:, h * half : (h + 1) * half].reshape(devices, 8, half)
                    sent[step, h, :, 2 * g + part] = piece
            if step == 0:
                @pl.when(g == 0)
                def _():
                    pl.semaphore_wait(barrier, devices - 1)
            for h in range(2):
                pair = sent[step, h, me, pl.ds(2 * g, 2)]
                held[step][h][pl.ds(me * planes + 2 * g, 2)] = pair
            to_all(
                lambda holder: sent.at[step, 0, holder, pl.ds(2 * g, 2)],
                held[step][0].at[pl.ds(me * planes + 2 * g, 2)],
                base,
            )
            return carry

        lax.fori_loop(0, own, one, 0)
        to_all(
            lambda holder: sent.at[step, 1, holder],
            held[step][1].at[pl.ds(me * planes, planes)],
            base + 1,
        )

    def evaluate(load):
        def chunk(c, carry):
            acc_re, acc_im = carry
            for u in range(unroll):
                q = c * unroll + u
                l, m, n = index_ref[0, q], index_ref[1, q], index_ref[2, q]
                w, keep = weight_ref[q], keep_ref[q]
                re, im = triple_product(
                    (load(l), load(l + 1)), (load(m), load(m + 1)), (load(n), load(n + 1))
                )
                acc_re = keep * acc_re - w * im
                acc_im = keep * acc_im + w * re
                partial[q, 0] = acc_re
                partial[q, 1] = acc_im
            return acc_re, acc_im

        zero = jnp.zeros((8, half), jnp.float32)
        lax.fori_loop(0, count // unroll, chunk, (zero, zero))

    def kerr(step, h, store):
        evaluate(lambda i: held[step][h][i])

        def combine(d, carry):
            for g in range(own):
                row = d * own + g
                place, has = last_ref[row], has_ref[row]
                for r in range(2):
                    i = d * planes + 2 * g + r
                    value = has * partial[place, r]
                    first[i] = value
                    mid[i] = held[step][h][i] + value
            return carry

        lax.fori_loop(0, devices, combine, 0)
        evaluate(lambda i: mid[i])

        def finish(d, carry):
            for g in range(own):
                row = d * own + g
                place, has = last_ref[row], has_ref[row]
                squares = [0.0, 0.0]
                for r in range(2):
                    i = d * planes + 2 * g + r
                    second = has * partial[place, r]
                    new = held[step][h][i] + 0.5 * (first[i] + second)
                    estimate = 0.5 * (second - first[i])
                    store(d, 2 * g + r, new)
                    squares[0] += estimate * estimate
                    squares[1] += new * new
                for kind in range(2):
                    total = jnp.sum(squares[kind], axis=0, keepdims=True)
                    if h == 0:
                        sums[kind, pl.ds(row, 1)] = total
                    else:
                        sums[kind, pl.ds(row, 1)] += total
            return carry

        lax.fori_loop(0, devices, finish, 0)

    def fold(step):
        for kind in range(2):
            norm[pl.ds(2 * step + kind, 1)] = jnp.sum(sums[kind].T, axis=0, keepdims=True)

    norm[...] = jnp.zeros_like(norm)
    spectral(lambda g: (x_ref[:, 0, g].reshape(radix, radix), x_ref[:, 1, g].reshape(radix, radix)), 0, 0)

    def keep_update(h):
        def store(d, plane, value):
            updated[h, d, plane] = value

        return store

    arrived(held[0][0].at[pl.ds(0, (devices - 1) * planes)], 0)
    kerr(0, 0, keep_update(0))
    back[0, me] = updated[0, me]
    to_all(lambda holder: updated.at[0, holder], back.at[0, me], 2)
    arrived(held[0][1].at[pl.ds(0, (devices - 1) * planes)], 1)
    kerr(0, 1, keep_update(1))
    back[1, me] = updated[1, me]
    for g in range(own):
        to_all(
            lambda holder: updated.at[1, holder, pl.ds(2 * g, 2)],
            back.at[1, me, pl.ds(2 * g, 2)],
            3 + g,
        )
    fold(0)
    arrived(back.at[0, pl.ds(0, devices - 1)], 2)

    def load_back(g):
        arrived(back.at[1, pl.ds(0, devices - 1), pl.ds(0, 2)], 3 + g)
        parts = []
        for r in range(2):
            parts.append(
                jnp.concatenate(
                    [back[h, :, 2 * g + r].reshape(radix, half) for h in range(2)], axis=1
                )
            )
        return parts

    base = 3 + own
    spectral(load_back, 1, base)

    def last_update(h):
        def store(d, plane, value):
            final[h, d // mode_ways, lax.rem(d, mode_ways), plane] = value

        return store

    def home(h, slot):
        def one(k, carry):
            mode = lax.rem(my_mode + k, mode_ways)
            pltpu.make_async_remote_copy(
                src_ref=final.at[h, :, mode],
                dst_ref=out_ref.at[h, my_mode],
                send_sem=send_sems.at[slot],
                recv_sem=recv_sems.at[slot],
                device_id=(mode, my_tm),
                device_id_type=MESH,
            ).start()
            return carry

        lax.fori_loop(1, mode_ways, one, 0)
        out_ref[h, my_mode] = final[h, :, my_mode]

    for h in range(2):
        arrived(held[1][h].at[pl.ds(0, (devices - 1) * planes)], base + h)
        kerr(1, h, last_update(h))
        home(h, base + 2 + h)
    fold(1)
    norms[me] = norm[...]
    to_all(lambda holder: norm, norms.at[me], base + 4)
    arrived(norms.at[pl.ds(0, devices - 1)], base + 4)
    total = jnp.sum(norms[...], axis=0)
    err_ref[...] = jnp.concatenate(
        [
            jnp.sqrt(total[2 * s : 2 * s + 1] / (total[2 * s + 1 : 2 * s + 2] + epsilon))
            for s in range(STEPS)
        ],
        axis=0,
    )
    for h in range(2):
        arrived(out_ref.at[h, pl.ds(0, mode_ways - 1)], base + 2 + h)
    for step, at in ((0, 0), (1, base)):
        for h in range(2):
            drained(sent.at[step, h, pl.ds(0, devices - 1)], at + h)
    drained(updated.at[0, pl.ds(0, devices - 1)], 2)
    for g in range(own):
        drained(updated.at[1, pl.ds(0, devices - 1), pl.ds(0, 2)], 3 + g)
    for h in range(2):
        drained(out_ref.at[h, pl.ds(0, mode_ways - 1)], base + 2 + h)
    drained(norms.at[pl.ds(0, devices - 1)], base + 4)


def step_all(ways, own, scalars, x, tables, twist, rotor):
    mode_ways, tm_ways = ways
    devices = mode_ways * tm_ways
    planes = 2 * own
    count = scalars[2].shape[0]
    half = twist.shape[1] // 2
    vmem = pl.BlockSpec(memory_space=pltpu.VMEM)
    smem = pl.BlockSpec(memory_space=pltpu.SMEM)
    real = lambda *shape: pltpu.VMEM(shape, jnp.float32)
    slots = 8 + own
    return pl.pallas_call(
        functools.partial(step_kernel, ways, own),
        in_specs=[smem] * 5 + [vmem] * 7,
        out_specs=[vmem, vmem],
        out_shape=[
            jax.ShapeDtypeStruct((2, mode_ways, tm_ways, planes, 8, half), jnp.float32),
            jax.ShapeDtypeStruct((STEPS, devices * own), jnp.float32),
        ],
        scratch_shapes=[
            real(2, 2, devices, planes, 8, half),
            *[real(devices * planes, 8, half)] * 4,
            real(devices * planes, 8, half),
            real(devices * planes, 8, half),
            real(count, 2, 8, half),
            real(2, devices, planes, 8, half),
            real(2, devices, planes, 8, half),
            real(2, tm_ways, mode_ways, planes, 8, half),
            real(2, devices * own, half),
            real(8, devices * own),
            real(devices, 8, devices * own),
            pltpu.SemaphoreType.DMA((slots,)),
            pltpu.SemaphoreType.DMA((slots,)),
        ],
        compiler_params=pltpu.CompilerParams(
            vmem_limit_bytes=56 * 1024 * 1024, collective_id=0, has_side_effects=True
        ),
        name="step_all",
    )(*scalars, x, *tables, twist, rotor)


def sorted_quartets(ways, own, quartets, intersections):
    mode_ways, tm_ways = ways
    modes_local = own * tm_ways
    modes_all = modes_local * mode_ways
    row = (quartets % modes_local // own * mode_ways + quartets // modes_local) * own
    row = row + quartets % own
    count = row.shape[1]
    place = lax.iota(jnp.int32, count)
    key = row[0] * count + place
    rank = jnp.sum((key[None, :] < key[:, None]).astype(jnp.int32), axis=1)
    pick = (rank[None, :] == place[:, None]).astype(jnp.float32)
    columns = jnp.concatenate([row.astype(jnp.float32), intersections[None]], axis=0)
    ordered = contract("iq,cq->ci", pick, columns)
    rows = jnp.round(ordered[:4]).astype(jnp.int32)
    keep = jnp.concatenate([jnp.zeros(1, bool), rows[0, 1:] == rows[0, :-1]])
    modes = lax.iota(jnp.int32, modes_all)
    below = jnp.sum((row[0][None, :] <= modes[:, None]).astype(jnp.int32), axis=1)
    has = jnp.any(row[0][None, :] == modes[:, None], axis=1)
    return (
        rows[1:] * 2,
        jnp.maximum(below - 1, 0),
        ordered[4],
        keep.astype(jnp.float32),
        has.astype(jnp.float32),
    )


def shards(ways, field, beta, quartets, intersections):
    mode_ways, tm_ways = ways
    _, modes_local, time_local = field.shape
    total_time = time_local * tm_ways
    radix = math.isqrt(total_time)
    own = modes_local // tm_ways
    tm_index = lax.axis_index("tm")

    table_re, table_im = dft_tables(radix)
    m1 = jnp.concatenate(
        [jnp.concatenate([table_re, -table_im], 1), jnp.concatenate([table_im, table_re], 1)], 0
    )
    m2 = jnp.concatenate(
        [jnp.concatenate([table_re, table_im], 1), jnp.concatenate([-table_im, table_re], 1)], 0
    )
    tables = split_table(m1) + split_table(m2)
    position = lax.iota(jnp.int32, radix)
    angle = (
        -2.0
        * math.pi
        / total_time
        * (position[:, None] * position[None, :] % total_time).astype(jnp.float32)
    )
    twist = jnp.stack([jnp.cos(angle), jnp.sin(angle)])
    wave = position[:, None] + radix * position[None, :]
    signed = jnp.where(wave < total_time // 2, wave, wave - total_time)
    frequency = signed.astype(jnp.float32) / (total_time / 2)
    mine = lax.dynamic_slice_in_dim(beta, tm_index * own, own, axis=1)
    phase = phase_of(
        mine[0][:, None, None], mine[1][:, None, None], mine[2][:, None, None], frequency[None]
    )
    rotor = jnp.stack([jnp.cos(phase), jnp.sin(phase)]) * (1.0 / total_time)
    scalars = sorted_quartets(ways, own, quartets, intersections)

    state = field.reshape(2, tm_ways, own, time_local // radix, radix).transpose(1, 0, 2, 3, 4)
    state = lax.all_to_all(state, "tm", split_axis=0, concat_axis=0, tiled=True)
    out, errors = step_all(ways, own, scalars, state, tables, twist, rotor)
    out = out.reshape(2, mode_ways, tm_ways, own, 2, 8, radix // 2)
    out = out.transpose(4, 2, 3, 1, 5, 0, 6).reshape(2, modes_local, time_local)
    errors = errors.reshape(STEPS, tm_ways, mode_ways, own)
    errors = lax.dynamic_index_in_dim(errors, lax.axis_index("mode"), axis=2, keepdims=False)
    return (out, errors.reshape(STEPS, modes_local))


def solution(mesh):
    placed = (P(None, "mode", "tm"), P(None, "mode"), P(), P())

    def body(field, beta, quartets, intersections):
        mode_ways, tm_ways = mesh.shape["mode"], mesh.shape["tm"]
        devices = mode_ways * tm_ways
        total_time = field.shape[2] * tm_ways
        fits = field.shape[1] % tm_ways == 0 and RADIX == 8 * devices
        if fits and total_time == RADIX * RADIX and field.shape[1] * mode_ways == 128:
            return shards((mode_ways, tm_ways), field, beta, quartets, intersections)
        return shards_general(field, beta, quartets, intersections)

    return jax.shard_map(
        body,
        mesh=mesh,
        in_specs=placed,
        out_specs=(P(None, "mode", "tm"), P(None, "mode")),
        check_vma=False,
    )
```

```python
import functools
import math

import jax
import jax.numpy as jnp
import numpy as np
from jax import lax
from jax.experimental import pallas as pl
from jax.experimental.pallas import tpu as pltpu
from jax.sharding import PartitionSpec as P

RADIX = 256
STEPS = 2


epsilon = 1e-06


def phase_of(offset, slope, curve, frequency):
    return math.pi * offset + 300.0 * slope * frequency + 3000.0 * curve * frequency * frequency


def triple_product(left_field, middle_field, conj_field):
    prod_re = left_field[0] * middle_field[0] - left_field[1] * middle_field[1]
    prod_im = left_field[0] * middle_field[1] + left_field[1] * middle_field[0]
    out_re = prod_re * conj_field[0] + prod_im * conj_field[1]
    out_im = prod_im * conj_field[0] - prod_re * conj_field[1]
    return (out_re, out_im)


def contract(form, first_operand, second_operand):
    return jnp.einsum(form, first_operand, second_operand, precision=lax.Precision.HIGHEST)


def rotate(real_part, imag_part, angle):
    cosine = jnp.cos(angle)
    sine_part = jnp.sin(angle)
    return (real_part * cosine - imag_part * sine_part, real_part * sine_part + imag_part * cosine)


def dft_tables(length):
    positions = lax.iota(jnp.int32, length)
    product = positions[:, None] * positions[None, :] % length
    angle = -2.0 * math.pi / length * product.astype(jnp.float32)
    return (jnp.cos(angle), jnp.sin(angle))


def to_columns(state):
    return lax.all_to_all(state, "tm", split_axis=3, concat_axis=2, tiled=True)


def to_rows(state):
    return lax.all_to_all(state, "tm", split_axis=2, concat_axis=3, tiled=True)


def linear_step(state, beta, table_re, table_im):
    radix_size = table_re.shape[0]
    total_time = radix_size * radix_size
    cols_local = state.shape[3]
    tm_index = lax.axis_index("tm")
    head_re = contract("ka,mab->mkb", table_re, state[0]) - contract(
        "ka,mab->mkb", table_im, state[1]
    )
    head_im = contract("ka,mab->mkb", table_re, state[1]) + contract(
        "ka,mab->mkb", table_im, state[0]
    )
    column = tm_index * cols_local + lax.iota(jnp.int32, cols_local)
    row_position = lax.iota(jnp.int32, radix_size)
    twist = (
        -2.0
        * math.pi
        / total_time
        * (row_position[:, None] * column[None, :] % total_time).astype(jnp.float32)
    )
    head_re, head_im = rotate(head_re, head_im, twist[None])
    turned = lax.all_to_all(
        jnp.stack([head_re, head_im]), "tm", split_axis=2, concat_axis=3, tiled=True
    )
    spec_re = contract("mcb,kb->mck", turned[0], table_re) - contract(
        "mcb,kb->mck", turned[1], table_im
    )
    spec_im = contract("mcb,kb->mck", turned[1], table_re) + contract(
        "mcb,kb->mck", turned[0], table_im
    )
    rows_local = turned.shape[2]
    first_index = tm_index * rows_local + lax.iota(jnp.int32, rows_local)
    wave = first_index[:, None] + radix_size * row_position[None, :]
    signed = jnp.where(wave < total_time // 2, wave, wave - total_time)
    frequency = signed.astype(jnp.float32) / (total_time / 2)
    angle = phase_of(
        beta[0][:, None, None], beta[1][:, None, None], beta[2][:, None, None], frequency[None]
    )
    spec_re, spec_im = rotate(spec_re, spec_im, angle)
    back_re = contract("mck,kb->mcb", spec_re, table_re) + contract(
        "mck,kb->mcb", spec_im, table_im
    )
    back_im = contract("mck,kb->mcb", spec_im, table_re) - contract(
        "mck,kb->mcb", spec_re, table_im
    )
    untwist = (
        2.0
        * math.pi
        / total_time
        * (first_index[:, None] * row_position[None, :] % total_time).astype(jnp.float32)
    )
    back_re, back_im = rotate(back_re, back_im, untwist[None])
    gathered = lax.all_to_all(
        jnp.stack([back_re, back_im]), "tm", split_axis=3, concat_axis=2, tiled=True
    )
    scale = 1.0 / total_time
    out_re = (
        contract("ka,mkb->mab", table_re, gathered[0])
        + contract("ka,mkb->mab", table_im, gathered[1])
    ) * scale
    out_im = (
        contract("ka,mkb->mab", table_re, gathered[1])
        - contract("ka,mkb->mab", table_im, gathered[0])
    ) * scale
    return jnp.stack([out_re, out_im])


def kerr_term(fields, quartets, intersections):
    count = quartets.shape[1]
    block_size = min(512, count)
    blocks = count // block_size
    grouped = quartets.reshape(4, blocks, block_size).transpose(1, 0, 2)
    weights = intersections.reshape(blocks, block_size)
    modes_all = fields.shape[1]
    mode_ids = lax.iota(jnp.int32, modes_all)

    def accumulate(running, block_item):
        indices, weight = block_item
        out_re, out_im = triple_product(
            jnp.take(fields, indices[1], axis=1),
            jnp.take(fields, indices[2], axis=1),
            jnp.take(fields, indices[3], axis=1),
        )
        owner = (indices[0][None, :] == mode_ids[:, None]).astype(jnp.float32) * weight[None, :]
        add_re = contract("pq,qt->pt", owner, -out_im)
        add_im = contract("pq,qt->pt", owner, out_re)
        return (running + jnp.stack([add_re, add_im]), None)

    running, unused = lax.scan(accumulate, jnp.zeros_like(fields), (grouped, weights))
    return running


def kerr_step(flat, quartets, intersections):
    spread = lax.all_to_all(flat, "mode", split_axis=2, concat_axis=1, tiled=True)
    first = kerr_term(spread, quartets, intersections)
    second = kerr_term(spread + first, quartets, intersections)
    updated = spread + 0.5 * (first + second)
    estimate = 0.5 * (second - first)
    returned, estimate_home = (
        lax.all_to_all(updated, "mode", split_axis=1, concat_axis=2, tiled=True),
        lax.all_to_all(estimate, "mode", split_axis=1, concat_axis=2, tiled=True),
    )
    error_part = jnp.sum(estimate_home * estimate_home, axis=(0, 2))
    field_part = jnp.sum(returned * returned, axis=(0, 2))
    return (returned, error_part, field_part)


def shards_general(field, beta, quartets, intersections):
    modes_local = field.shape[1]
    time_local = field.shape[2]
    table_re, table_im = dft_tables(RADIX)
    state = field.reshape(2, modes_local, time_local // RADIX, RADIX)
    state = to_columns(state)
    error_rows = []
    for step_index in range(STEPS):
        columns = state
        columns = linear_step(columns, beta, table_re, table_im)
        updated, error_part, field_part = kerr_step(
            columns.reshape(2, modes_local, time_local), quartets, intersections
        )
        error_sq, field_sq = lax.psum((error_part, field_part), "tm")
        error_rows.append(jnp.sqrt(error_sq / (field_sq + epsilon)))
        state = updated.reshape(columns.shape)
    state = to_rows(state)
    errors = jnp.stack(error_rows)
    return (state.reshape(2, modes_local, time_local), errors)


UNROLL = 8
MESH = pl.DeviceIdType.MESH


def half_pi_terms():
    whole = math.pi / 2
    first = math.floor(whole * 2**11) / 2**11
    second = math.floor((whole - first) * 2**23) / 2**23
    return first, second, whole - first - second


HALF_PI = half_pi_terms()


def split(value):
    high = value.astype(jnp.bfloat16)
    low = (value - high.astype(jnp.float32)).astype(jnp.bfloat16)
    return high, low


def split_table(value):
    high = lax.reduce_precision(value, exponent_bits=8, mantissa_bits=7)
    return high.astype(jnp.bfloat16), (value - high).astype(jnp.bfloat16)


def product(left, right):
    dot = lambda a, b: jnp.dot(a, b, preferred_element_type=jnp.float32)
    return dot(left[0], right[0]) + (dot(left[0], right[1]) + dot(left[1], right[0]))


def transform(real, imag, m1, m2, twist_ref, ro_re, ro_im):
    radix = twist_ref.shape[1]
    head = product(m1, split(jnp.concatenate([real, imag], axis=0)))
    head_re, head_im = head[:radix], head[radix:]
    tw_re, tw_im = twist_ref[0], twist_ref[1]
    re = head_re * tw_re - head_im * tw_im
    im = head_re * tw_im + head_im * tw_re
    spec = product(split(jnp.concatenate([re, im], axis=1)), m2)
    spec_re, spec_im = spec[:, :radix], spec[:, radix:]
    re = spec_re * ro_re - spec_im * ro_im
    im = spec_re * ro_im + spec_im * ro_re
    back = product(split(jnp.concatenate([re, im], axis=1)), m1)
    back_re, back_im = back[:, :radix], back[:, radix:]
    re = back_re * tw_re + back_im * tw_im
    im = back_im * tw_re - back_re * tw_im
    out = product(m2, split(jnp.concatenate([re, im], axis=0)))
    return out[:radix], out[radix:]


def cos_sin(angle):
    turns = jnp.round(angle * (2.0 / math.pi))
    rest = angle - turns * HALF_PI[0]
    rest = rest - turns * HALF_PI[1]
    rest = rest - turns * HALF_PI[2]
    square = rest * rest
    sine = -1.9515295891e-4 * square + 8.3321608736e-3
    sine = (sine * square - 1.6666654611e-1) * square * rest + rest
    cosine = 2.443315711809948e-5 * square - 1.388731625493765e-3
    cosine = (cosine * square + 4.166664568298827e-2) * square * square - 0.5 * square + 1.0
    quarter = turns.astype(jnp.int32)
    odd = (quarter & 1) == 1
    cos_part = jnp.where(odd, sine, cosine)
    sin_part = jnp.where(odd, cosine, sine)
    cos_part = jnp.where(((quarter + 1) & 2) == 2, -cos_part, cos_part)
    sin_part = jnp.where((quarter & 2) == 2, -sin_part, sin_part)
    return cos_part, sin_part


def step_kernel(
    ways, own, beta_ref, quartets_ref, intersections_ref, x_ref, table_ref, twist_ref,
    out_ref, err_ref,
    m1h, m1l, m2h, m2l, rotor_ref, staged, columns,
    sent, held_00, held_01, held_10, held_11, mid, first, partial, updated, back, final, sums, norm, norms,
    places, shares, spread_ref, weight_ref, keep_ref, left_ref, middle_ref, right_ref, last_ref, has_ref,
    send_sems, recv_sems, table_sems,
):
    mode_ways, tm_ways = ways
    devices = mode_ways * tm_ways
    planes = 2 * own
    held = ((held_00, held_01), (held_10, held_11))
    my_mode, my_tm = lax.axis_index("mode"), lax.axis_index("tm")
    me = my_tm * mode_ways + my_mode
    radix = twist_ref.shape[1]
    half = radix // 2
    count = weight_ref.shape[0]
    modes_local = own * tm_ways
    unroll = UNROLL if count % UNROLL == 0 else 1
    total_time = radix * radix
    rows_local = radix // tm_ways
    head = 8 + own
    octets = x_ref.shape[1]

    def partner(k):
        tm = lax.rem(my_tm + lax.rem(k, tm_ways), tm_ways)
        mode = lax.rem(my_mode + k // tm_ways, mode_ways)
        return mode, tm, tm * mode_ways + mode

    barrier = pltpu.get_barrier_semaphore()

    def greet(k, carry):
        mode, tm, _ = partner(k)
        pl.semaphore_signal(barrier, inc=1, device_id=(mode, tm), device_id_type=MESH)
        return carry

    lax.fori_loop(1, devices, greet, 0)

    def to_all(pick_src, dst, slot):
        def one(k, carry):
            mode, tm, holder = partner(k)
            pltpu.make_async_remote_copy(
                src_ref=pick_src(holder),
                dst_ref=dst,
                send_sem=send_sems.at[slot],
                recv_sem=recv_sems.at[slot],
                device_id=(mode, tm),
                device_id_type=MESH,
            ).start()
            return carry

        lax.fori_loop(1, devices, one, 0)

    def arrived(ref, slot):
        pltpu.make_async_copy(ref, ref, recv_sems.at[slot]).wait()

    def drained(ref, slot):
        pltpu.make_async_copy(ref, ref, send_sems.at[slot]).wait()

    def spectral(load, step, base):
        m1, m2 = (m1h[...], m1l[...]), (m2h[...], m2l[...])

        def one(g, carry):
            if step == 0:
                make_rotor(g)
            real, imag = load(g)
            re, im = transform(real, imag, m1, m2, twist_ref, rotor_ref[0, g], rotor_ref[1, g])
            for part, value in enumerate((re, im)):
                for h in range(2):
                    piece = value[:, h * half : (h + 1) * half].reshape(devices, 8, half)
                    sent[step, h, :, 2 * g + part] = piece
            for h in range(2):
                pair = sent[step, h, me, pl.ds(2 * g, 2)]
                held[step][h][pl.ds(me * planes + 2 * g, 2)] = pair
            to_all(
                lambda holder: sent.at[step, 0, holder, pl.ds(2 * g, 2)],
                held[step][0].at[pl.ds(me * planes + 2 * g, 2)],
                base,
            )
            return carry

        lax.fori_loop(0, own, one, 0)
        to_all(
            lambda holder: sent.at[step, 1, holder],
            held[step][1].at[pl.ds(me * planes, planes)],
            base + 1,
        )

    def order_quartets():
        quartet = quartets_ref[...]
        row = (quartet % modes_local // own * mode_ways + quartet // modes_local) * own
        row = row + quartet % own
        position = lax.broadcasted_iota(jnp.int32, (1, count), 1)
        lane = lax.broadcasted_iota(jnp.int32, (1, half), 1)
        spread = lambda line: jnp.broadcast_to(line, (half, count)).T
        key = row[0:1] * count + position
        places[4:5] = key
        spread_ref[4] = spread(key)
        for i in range(4):
            spread_ref[i] = spread(row[i : i + 1])
        weight_ref[...] = spread(intersections_ref[...])
        gather = lambda mask, values: jnp.sum(
            jnp.where(mask, values, jnp.zeros_like(values)), axis=0, keepdims=True
        )

        def rank_block(b, carry):
            here = pl.ds(pl.multiple_of(b * half, half), half)
            before = spread_ref[4] < places[4:5, here]
            places[5:6, here] = gather(before, jnp.ones((count, half), jnp.int32))
            return carry

        lax.fori_loop(0, count // half, rank_block, 0)
        spread_ref[4] = spread(places[5:6])

        def place_block(b, carry):
            here = pl.ds(pl.multiple_of(b * half, half), half)
            hit = spread_ref[4] == lane + b * half
            for i in range(4):
                places[i : i + 1, here] = gather(hit, spread_ref[i])
            shares[1:2, here] = gather(hit, weight_ref[...])
            return carry

        lax.fori_loop(0, count // half, place_block, 0)
        ones = jnp.ones((count, half), jnp.int32)
        below = gather(spread_ref[0] <= lane, ones)
        equal = gather(spread_ref[0] == lane, ones)
        places[4:5, :half] = jnp.maximum(below - 1, 0)
        shares[0:1, :half] = jnp.where(equal > 0, 1.0, 0.0)
        owner = places[0:1]
        same = jnp.logical_and(owner == pltpu.roll(owner, 1, 1), position > 0)
        keep_ref[...] = spread(jnp.where(same, 1.0, 0.0))
        weight_ref[...] = spread(shares[1:2])
        for i in range(1, 4):
            places[i : i + 1] = places[i : i + 1] * 2
        copies = [
            pltpu.make_async_copy(places.at[1 + i], ref, table_sems.at[i])
            for i, ref in enumerate((left_ref, middle_ref, right_ref))
        ]
        copies.append(
            pltpu.make_async_copy(places.at[4, pl.ds(0, half)], last_ref, table_sems.at[3])
        )
        copies.append(pltpu.make_async_copy(shares.at[0, pl.ds(0, half)], has_ref, table_sems.at[4]))
        for copy in copies:
            copy.start()
        for copy in copies:
            copy.wait()

    def evaluate(source):
        load = lambda plane: (source[plane], source[plane + 1])

        def chunk(c, carry):
            acc_re, acc_im = carry
            for u in range(unroll):
                q = c * unroll + u
                re, im = triple_product(
                    load(left_ref[q]), load(middle_ref[q]), load(right_ref[q])
                )
                w = jnp.broadcast_to(weight_ref[pl.ds(q, 1), :], (8, half))
                keep = jnp.broadcast_to(keep_ref[pl.ds(q, 1), :], (8, half))
                acc_re = keep * acc_re - w * im
                acc_im = keep * acc_im + w * re
                partial[q, 0] = acc_re
                partial[q, 1] = acc_im
            return acc_re, acc_im

        zero = jnp.zeros((8, half), jnp.float32)
        lax.fori_loop(0, count // unroll, chunk, (zero, zero))

    def kerr(step, h, store):
        evaluate(held[step][h])

        def combine(d, carry):
            for g in range(own):
                row = d * own + g
                place, has = last_ref[row], has_ref[row]
                for r in range(2):
                    i = d * planes + 2 * g + r
                    value = has * partial[place, r]
                    first[i] = value
                    mid[i] = held[step][h][i] + value
            return carry

        lax.fori_loop(0, devices, combine, 0)
        evaluate(mid)

        def finish(d, carry):
            for g in range(own):
                row = d * own + g
                place, has = last_ref[row], has_ref[row]
                squares = [0.0, 0.0]
                for r in range(2):
                    i = d * planes + 2 * g + r
                    second = has * partial[place, r]
                    new = held[step][h][i] + 0.5 * (first[i] + second)
                    estimate = 0.5 * (second - first[i])
                    store(d, 2 * g + r, new)
                    squares[0] += estimate * estimate
                    squares[1] += new * new
                for kind in range(2):
                    total = jnp.sum(squares[kind], axis=0, keepdims=True)
                    if h == 0:
                        sums[kind, pl.ds(row, 1)] = total
                    else:
                        sums[kind, pl.ds(row, 1)] += total
            return carry

        lax.fori_loop(0, devices, finish, 0)

    def fold(step):
        for kind in range(2):
            norm[pl.ds(2 * step + kind, 1)] = jnp.sum(sums[kind].T, axis=0, keepdims=True)

    norm[...] = jnp.zeros_like(norm)
    for g in range(own):
        for t in range(tm_ways):
            octet, line = divmod(t * own + g, 8)
            for r in range(2):
                for side in range(2):
                    rows = pl.ds(line + 8 * side, rows_local, stride=16)
                    staged[g, t, r, side] = x_ref[r, octet, rows, :]
        if g == 0:
            pl.semaphore_wait(barrier, devices - 1)
        columns[g, my_tm] = staged[g, my_tm]

        def fetch(k, carry, g=g):
            tm = lax.rem(my_tm + k, tm_ways)
            pltpu.make_async_remote_copy(
                src_ref=staged.at[g, tm],
                dst_ref=columns.at[g, my_tm],
                send_sem=send_sems.at[head + g],
                recv_sem=recv_sems.at[head + g],
                device_id=(my_mode, tm),
                device_id_type=MESH,
            ).start()
            return carry

        lax.fori_loop(1, tm_ways, fetch, 0)

    for part, (m1, m2) in enumerate(((m1h, m2h), (m1l, m2l))):
        re, im = table_ref[part, 0], table_ref[part, 1]
        for table, sign in ((m1, 1), (m2, -1)):
            table[:radix, :radix] = re
            table[radix:, radix:] = re
            table[:radix, radix:] = -im if sign == 1 else im
            table[radix:, :radix] = im if sign == 1 else -im

    order_quartets()

    def make_rotor(g):
        mode = my_tm * own + g
        offset, slope, curve = (beta_ref[i, mode] for i in range(3))
        offset, slope, curve = math.pi * offset, 300.0 * slope, 3000.0 * curve

        def strip(c, carry):
            start = pl.multiple_of(8 * c, 8)
            row = lax.broadcasted_iota(jnp.int32, (8, radix), 0) + start
            wave = row + radix * lax.broadcasted_iota(jnp.int32, (8, radix), 1)
            signed = jnp.where(wave < total_time // 2, wave, wave - total_time)
            frequency = signed.astype(jnp.float32) * (2.0 / total_time)
            phase = offset + slope * frequency + curve * frequency * frequency
            cosine, sine = cos_sin(phase)
            rotor_ref[0, g, pl.ds(start, 8)] = cosine * (1.0 / total_time)
            rotor_ref[1, g, pl.ds(start, 8)] = sine * (1.0 / total_time)
            return carry

        lax.fori_loop(0, radix // 8, strip, 0, unroll=4)

    def load_columns(g):
        arrived(columns.at[g, pl.ds(0, tm_ways - 1)], head + g)
        return [
            jnp.concatenate(
                [columns[g, :, r, side].reshape(radix, half) for side in range(2)], axis=1
            )
            for r in range(2)
        ]

    spectral(load_columns, 0, 0)

    def keep_update(h):
        def store(d, plane, value):
            updated[h, d, plane] = value

        return store

    arrived(held[0][0].at[pl.ds(0, (devices - 1) * planes)], 0)
    kerr(0, 0, keep_update(0))
    back[0, me] = updated[0, me]
    to_all(lambda holder: updated.at[0, holder], back.at[0, me], 2)
    arrived(held[0][1].at[pl.ds(0, (devices - 1) * planes)], 1)
    kerr(0, 1, keep_update(1))
    back[1, me] = updated[1, me]
    for g in range(own):
        to_all(
            lambda holder: updated.at[1, holder, pl.ds(2 * g, 2)],
            back.at[1, me, pl.ds(2 * g, 2)],
            3 + g,
        )
    fold(0)
    arrived(back.at[0, pl.ds(0, devices - 1)], 2)

    def load_back(g):
        arrived(back.at[1, pl.ds(0, devices - 1), pl.ds(0, 2)], 3 + g)
        parts = []
        for r in range(2):
            parts.append(
                jnp.concatenate(
                    [back[h, :, 2 * g + r].reshape(radix, half) for h in range(2)], axis=1
                )
            )
        return parts

    base = 3 + own
    spectral(load_back, 1, base)

    def last_update(h):
        def store(d, plane, value):
            g, r = divmod(plane, 2)
            mode = d // mode_ways * own + g
            rows = pl.ds(lax.rem(mode, 8), 8, stride=8)
            final.reshape(2, mode_ways, 2, octets, 64, half)[
                h, lax.rem(d, mode_ways), r, mode // 8, rows, :
            ] = value

        return store

    def home(h, slot):
        def one(k, carry):
            mode = lax.rem(my_mode + k, mode_ways)
            pltpu.make_async_remote_copy(
                src_ref=final.at[h, mode],
                dst_ref=out_ref.at[:, :, my_mode, :, h],
                send_sem=send_sems.at[slot],
                recv_sem=recv_sems.at[slot],
                device_id=(mode, my_tm),
                device_id_type=MESH,
            ).start()
            return carry

        lax.fori_loop(1, mode_ways, one, 0)
        out_ref[:, :, my_mode, :, h] = final[h, my_mode]

    for h in range(2):
        arrived(held[1][h].at[pl.ds(0, (devices - 1) * planes)], base + h)
        kerr(1, h, last_update(h))
        home(h, base + 2 + h)
    fold(1)
    norms[me] = norm[...]
    to_all(lambda holder: norm, norms.at[me], base + 4)
    arrived(norms.at[pl.ds(0, devices - 1)], base + 4)
    total = jnp.sum(norms[...], axis=0)
    mode = lax.broadcasted_iota(jnp.int32, (devices * own, modes_local), 1)
    place = lax.broadcasted_iota(jnp.int32, (devices * own, modes_local), 0)
    pick = place == (mode // own * mode_ways + my_mode) * own + mode % own
    total = contract("ij,jk->ik", total, jnp.where(pick, 1.0, 0.0))
    err_ref[...] = jnp.concatenate(
        [
            jnp.sqrt(total[2 * s : 2 * s + 1] / (total[2 * s + 1 : 2 * s + 2] + epsilon))
            for s in range(STEPS)
        ],
        axis=0,
    )
    for h in range(2):
        arrived(final.at[h, pl.ds(0, mode_ways - 1)], base + 2 + h)
    for step, at in ((0, 0), (1, base)):
        for h in range(2):
            drained(sent.at[step, h, pl.ds(0, devices - 1)], at + h)
    drained(updated.at[0, pl.ds(0, devices - 1)], 2)
    for g in range(own):
        drained(updated.at[1, pl.ds(0, devices - 1), pl.ds(0, 2)], 3 + g)
    for h in range(2):
        drained(final.at[h, pl.ds(0, mode_ways - 1)], base + 2 + h)
    for g in range(own):
        drained(columns.at[g, pl.ds(0, tm_ways - 1)], head + g)
    drained(norms.at[pl.ds(0, devices - 1)], base + 4)


def step_all(ways, own, beta, quartets, intersections, x, table, twist):
    mode_ways, tm_ways = ways
    devices = mode_ways * tm_ways
    planes = 2 * own
    count = quartets.shape[1]
    radix = twist.shape[1]
    half = radix // 2
    octets = x.shape[1]
    vmem = pl.BlockSpec(memory_space=pltpu.VMEM)
    smem = pl.BlockSpec(memory_space=pltpu.SMEM)
    real = lambda *shape: pltpu.VMEM(shape, jnp.float32)
    slots = 8 + 2 * own
    return pl.pallas_call(
        functools.partial(step_kernel, ways, own),
        in_specs=[smem] + [vmem] * 5,
        out_specs=[vmem, vmem],
        out_shape=[
            jax.ShapeDtypeStruct((2, octets, mode_ways, 8, 2, 8, half), jnp.float32),
            jax.ShapeDtypeStruct((STEPS, own * tm_ways), jnp.float32),
        ],
        scratch_shapes=[
            *[pltpu.VMEM((2 * radix, 2 * radix), jnp.bfloat16)] * 4,
            real(2, own, radix, radix),
            real(own, tm_ways, 2, 2, radix // tm_ways, half),
            real(own, tm_ways, 2, 2, radix // tm_ways, half),
            real(2, 2, devices, planes, 8, half),
            *[real(devices * planes, 8, half)] * 4,
            real(devices * planes, 8, half),
            real(devices * planes, 8, half),
            real(count, 2, 8, half),
            real(2, devices, planes, 8, half),
            real(2, devices, planes, 8, half),
            real(2, mode_ways, 2, octets, 8, 8, half),
            real(2, devices * own, half),
            real(8, devices * own),
            real(devices, 8, devices * own),
            pltpu.VMEM((8, count), jnp.int32),
            real(2, count),
            pltpu.VMEM((5, count, half), jnp.int32),
            real(count, half),
            real(count, half),
            *[pltpu.SMEM((count,), jnp.int32)] * 3,
            pltpu.SMEM((half,), jnp.int32),
            pltpu.SMEM((half,), jnp.float32),
            pltpu.SemaphoreType.DMA((slots,)),
            pltpu.SemaphoreType.DMA((slots,)),
            pltpu.SemaphoreType.DMA((5,)),
        ],
        compiler_params=pltpu.CompilerParams(
            vmem_limit_bytes=56 * 1024 * 1024, collective_id=0, has_side_effects=True
        ),
        name="step_all",
    )(beta, quartets, intersections[None], x, table, twist)


def constant_tables(radix):
    position = np.arange(radix)
    product_of = position[:, None] * position[None, :]
    angle = -2.0 * np.pi / radix * (product_of % radix)
    table = np.stack([np.cos(angle), np.sin(angle)]).astype(np.float32)
    high = table.astype(jnp.bfloat16)
    low = (table - high.astype(np.float32)).astype(jnp.bfloat16)
    turn = -2.0 * np.pi / radix**2 * product_of
    twist = np.stack([np.cos(turn), np.sin(turn)]).astype(np.float32)
    return jnp.asarray(np.stack([high, low])), jnp.asarray(twist)


def shards(ways, field, beta, quartets, intersections):
    mode_ways, tm_ways = ways
    _, modes_local, time_local = field.shape
    radix = math.isqrt(time_local * tm_ways)
    own = modes_local // tm_ways
    table, twist = constant_tables(radix)
    octets, tiles = modes_local // 8, time_local // 128
    x = field.reshape(2, octets, 8, tiles, 128).transpose(0, 1, 3, 2, 4)
    x = x.reshape(2, octets, tiles * 8, 128)
    out, errors = step_all(ways, own, beta, quartets, intersections, x, table, twist)
    out = out.reshape(2, octets, tiles, 8, 128).transpose(0, 1, 3, 2, 4)
    return (out.reshape(2, modes_local, time_local), errors)


def solution(mesh):
    placed = (P(None, "mode", "tm"), P(None, "mode"), P(), P())

    def body(field, beta, quartets, intersections):
        mode_ways, tm_ways = mesh.shape["mode"], mesh.shape["tm"]
        devices = mode_ways * tm_ways
        total_time = field.shape[2] * tm_ways
        fits = field.shape[1] % tm_ways == 0 and RADIX == 8 * devices
        fits = fits and field.shape[1] % 8 == 0 and quartets.shape[1] % 128 == 0
        if fits and total_time == RADIX * RADIX and field.shape[1] * mode_ways == 128:
            return shards((mode_ways, tm_ways), field, beta, quartets, intersections)
        return shards_general(field, beta, quartets, intersections)

    return jax.shard_map(
        body,
        mesh=mesh,
        in_specs=placed,
        out_specs=(P(None, "mode", "tm"), P(None, "mode")),
        check_vma=False,
    )
```

```python
import functools
import math

import jax
import jax.numpy as jnp
import numpy as np
from jax import lax
from jax.experimental import pallas as pl
from jax.experimental.pallas import tpu as pltpu
from jax.sharding import PartitionSpec as P

RADIX = 256
STEPS = 2


epsilon = 1e-06


def phase_of(offset, slope, curve, frequency):
    return math.pi * offset + 300.0 * slope * frequency + 3000.0 * curve * frequency * frequency


def triple_product(left_field, middle_field, conj_field):
    prod_re = left_field[0] * middle_field[0] - left_field[1] * middle_field[1]
    prod_im = left_field[0] * middle_field[1] + left_field[1] * middle_field[0]
    out_re = prod_re * conj_field[0] + prod_im * conj_field[1]
    out_im = prod_im * conj_field[0] - prod_re * conj_field[1]
    return (out_re, out_im)


def contract(form, first_operand, second_operand):
    return jnp.einsum(form, first_operand, second_operand, precision=lax.Precision.HIGHEST)


def rotate(real_part, imag_part, angle):
    cosine = jnp.cos(angle)
    sine_part = jnp.sin(angle)
    return (real_part * cosine - imag_part * sine_part, real_part * sine_part + imag_part * cosine)


def dft_tables(length):
    positions = lax.iota(jnp.int32, length)
    product = positions[:, None] * positions[None, :] % length
    angle = -2.0 * math.pi / length * product.astype(jnp.float32)
    return (jnp.cos(angle), jnp.sin(angle))


def to_columns(state):
    return lax.all_to_all(state, "tm", split_axis=3, concat_axis=2, tiled=True)


def to_rows(state):
    return lax.all_to_all(state, "tm", split_axis=2, concat_axis=3, tiled=True)


def linear_step(state, beta, table_re, table_im):
    radix_size = table_re.shape[0]
    total_time = radix_size * radix_size
    cols_local = state.shape[3]
    tm_index = lax.axis_index("tm")
    head_re = contract("ka,mab->mkb", table_re, state[0]) - contract(
        "ka,mab->mkb", table_im, state[1]
    )
    head_im = contract("ka,mab->mkb", table_re, state[1]) + contract(
        "ka,mab->mkb", table_im, state[0]
    )
    column = tm_index * cols_local + lax.iota(jnp.int32, cols_local)
    row_position = lax.iota(jnp.int32, radix_size)
    twist = (
        -2.0
        * math.pi
        / total_time
        * (row_position[:, None] * column[None, :] % total_time).astype(jnp.float32)
    )
    head_re, head_im = rotate(head_re, head_im, twist[None])
    turned = lax.all_to_all(
        jnp.stack([head_re, head_im]), "tm", split_axis=2, concat_axis=3, tiled=True
    )
    spec_re = contract("mcb,kb->mck", turned[0], table_re) - contract(
        "mcb,kb->mck", turned[1], table_im
    )
    spec_im = contract("mcb,kb->mck", turned[1], table_re) + contract(
        "mcb,kb->mck", turned[0], table_im
    )
    rows_local = turned.shape[2]
    first_index = tm_index * rows_local + lax.iota(jnp.int32, rows_local)
    wave = first_index[:, None] + radix_size * row_position[None, :]
    signed = jnp.where(wave < total_time // 2, wave, wave - total_time)
    frequency = signed.astype(jnp.float32) / (total_time / 2)
    angle = phase_of(
        beta[0][:, None, None], beta[1][:, None, None], beta[2][:, None, None], frequency[None]
    )
    spec_re, spec_im = rotate(spec_re, spec_im, angle)
    back_re = contract("mck,kb->mcb", spec_re, table_re) + contract(
        "mck,kb->mcb", spec_im, table_im
    )
    back_im = contract("mck,kb->mcb", spec_im, table_re) - contract(
        "mck,kb->mcb", spec_re, table_im
    )
    untwist = (
        2.0
        * math.pi
        / total_time
        * (first_index[:, None] * row_position[None, :] % total_time).astype(jnp.float32)
    )
    back_re, back_im = rotate(back_re, back_im, untwist[None])
    gathered = lax.all_to_all(
        jnp.stack([back_re, back_im]), "tm", split_axis=3, concat_axis=2, tiled=True
    )
    scale = 1.0 / total_time
    out_re = (
        contract("ka,mkb->mab", table_re, gathered[0])
        + contract("ka,mkb->mab", table_im, gathered[1])
    ) * scale
    out_im = (
        contract("ka,mkb->mab", table_re, gathered[1])
        - contract("ka,mkb->mab", table_im, gathered[0])
    ) * scale
    return jnp.stack([out_re, out_im])


def kerr_term(fields, quartets, intersections):
    count = quartets.shape[1]
    block_size = min(512, count)
    blocks = count // block_size
    grouped = quartets.reshape(4, blocks, block_size).transpose(1, 0, 2)
    weights = intersections.reshape(blocks, block_size)
    modes_all = fields.shape[1]
    mode_ids = lax.iota(jnp.int32, modes_all)

    def accumulate(running, block_item):
        indices, weight = block_item
        out_re, out_im = triple_product(
            jnp.take(fields, indices[1], axis=1),
            jnp.take(fields, indices[2], axis=1),
            jnp.take(fields, indices[3], axis=1),
        )
        owner = (indices[0][None, :] == mode_ids[:, None]).astype(jnp.float32) * weight[None, :]
        add_re = contract("pq,qt->pt", owner, -out_im)
        add_im = contract("pq,qt->pt", owner, out_re)
        return (running + jnp.stack([add_re, add_im]), None)

    running, unused = lax.scan(accumulate, jnp.zeros_like(fields), (grouped, weights))
    return running


def kerr_step(flat, quartets, intersections):
    spread = lax.all_to_all(flat, "mode", split_axis=2, concat_axis=1, tiled=True)
    first = kerr_term(spread, quartets, intersections)
    second = kerr_term(spread + first, quartets, intersections)
    updated = spread + 0.5 * (first + second)
    estimate = 0.5 * (second - first)
    returned, estimate_home = (
        lax.all_to_all(updated, "mode", split_axis=1, concat_axis=2, tiled=True),
        lax.all_to_all(estimate, "mode", split_axis=1, concat_axis=2, tiled=True),
    )
    error_part = jnp.sum(estimate_home * estimate_home, axis=(0, 2))
    field_part = jnp.sum(returned * returned, axis=(0, 2))
    return (returned, error_part, field_part)


def shards_general(field, beta, quartets, intersections):
    modes_local = field.shape[1]
    time_local = field.shape[2]
    table_re, table_im = dft_tables(RADIX)
    state = field.reshape(2, modes_local, time_local // RADIX, RADIX)
    state = to_columns(state)
    error_rows = []
    for step_index in range(STEPS):
        columns = state
        columns = linear_step(columns, beta, table_re, table_im)
        updated, error_part, field_part = kerr_step(
            columns.reshape(2, modes_local, time_local), quartets, intersections
        )
        error_sq, field_sq = lax.psum((error_part, field_part), "tm")
        error_rows.append(jnp.sqrt(error_sq / (field_sq + epsilon)))
        state = updated.reshape(columns.shape)
    state = to_rows(state)
    errors = jnp.stack(error_rows)
    return (state.reshape(2, modes_local, time_local), errors)


UNROLL = 32
MESH = pl.DeviceIdType.MESH


def half_pi_terms():
    whole = math.pi / 2
    first = math.floor(whole * 2**11) / 2**11
    second = math.floor((whole - first) * 2**23) / 2**23
    return first, second, whole - first - second


HALF_PI = half_pi_terms()


def split(value):
    high = value.astype(jnp.bfloat16)
    low = (value - high.astype(jnp.float32)).astype(jnp.bfloat16)
    return high, low


def split_table(value):
    high = lax.reduce_precision(value, exponent_bits=8, mantissa_bits=7)
    return high.astype(jnp.bfloat16), (value - high).astype(jnp.bfloat16)


def product(left, right):
    dot = lambda a, b: jnp.dot(a, b, preferred_element_type=jnp.float32)
    return dot(left[0], right[0]) + (dot(left[0], right[1]) + dot(left[1], right[0]))


def transform(real, imag, m1, m2, twist_ref, ro_re, ro_im):
    radix = twist_ref.shape[1]
    head = product(m1, split(jnp.concatenate([real, imag], axis=0)))
    head_re, head_im = head[:radix], head[radix:]
    tw_re, tw_im = twist_ref[0], twist_ref[1]
    re = head_re * tw_re - head_im * tw_im
    im = head_re * tw_im + head_im * tw_re
    spec = product(split(jnp.concatenate([re, im], axis=1)), m2)
    spec_re, spec_im = spec[:, :radix], spec[:, radix:]
    re = spec_re * ro_re - spec_im * ro_im
    im = spec_re * ro_im + spec_im * ro_re
    back = product(split(jnp.concatenate([re, im], axis=1)), m1)
    back_re, back_im = back[:, :radix], back[:, radix:]
    re = back_re * tw_re + back_im * tw_im
    im = back_im * tw_re - back_re * tw_im
    out = product(m2, split(jnp.concatenate([re, im], axis=0)))
    return out[:radix], out[radix:]


def cos_sin(angle):
    turns = jnp.round(angle * (2.0 / math.pi))
    rest = angle - turns * HALF_PI[0]
    rest = rest - turns * HALF_PI[1]
    rest = rest - turns * HALF_PI[2]
    square = rest * rest
    sine = -1.9515295891e-4 * square + 8.3321608736e-3
    sine = (sine * square - 1.6666654611e-1) * square * rest + rest
    cosine = 2.443315711809948e-5 * square - 1.388731625493765e-3
    cosine = (cosine * square + 4.166664568298827e-2) * square * square - 0.5 * square + 1.0
    quarter = turns.astype(jnp.int32)
    odd = (quarter & 1) == 1
    cos_part = jnp.where(odd, sine, cosine)
    sin_part = jnp.where(odd, cosine, sine)
    cos_part = jnp.where(((quarter + 1) & 2) == 2, -cos_part, cos_part)
    sin_part = jnp.where((quarter & 2) == 2, -sin_part, sin_part)
    return cos_part, sin_part


def step_kernel(
    ways, own, beta_ref, quartets_ref, intersections_ref, x_hbm, table_hbm, twist_hbm,
    out_ref, err_ref,
    x_ref, table_ref, twist_ref,
    m1h, m1l, m2h, m2l, rotor_ref, staged, columns,
    sent, short, relay, held_00, held_01, held_10, held_11, held_12, mid, first, partial, updated, back, final, sums, norm, norms,
    places, shares, spread_ref, weight_ref, keep_ref, left_ref, middle_ref, right_ref, last_ref, has_ref,
    send_sems, recv_sems, table_sems, own_sems,
):
    mode_ways, tm_ways = ways
    devices = mode_ways * tm_ways
    planes = 2 * own
    my_mode, my_tm = lax.axis_index("mode"), lax.axis_index("tm")
    me = my_tm * mode_ways + my_mode
    radix = twist_ref.shape[1]
    half = radix // 2
    parts = (
        ((sent.at[0], held_00, 0, 0, 8), (sent.at[1], held_01, 1, 0, 8)),
        (
            (sent.at[2], held_10, 0, 0, 8),
            (short.at[0].reshape(devices, planes, 4, half), held_11, 1, 0, 4),
            (short.at[1].reshape(devices, planes, 4, half), held_12, 1, 4, 4),
        ),
    )
    count = weight_ref.shape[0]
    modes_local = own * tm_ways
    unroll = UNROLL if count % UNROLL == 0 else 1
    total_time = radix * radix
    rows_local = radix // tm_ways
    slot_back, slot_last = 2, 3 + own
    slot_home, slot_norm, head = slot_last + 3, slot_last + 6, slot_last + 7
    slot_relay = head + own
    octets = x_ref.shape[1]

    def partner(k):
        tm = lax.rem(my_tm + lax.rem(k, tm_ways), tm_ways)
        mode = lax.rem(my_mode + k // tm_ways, mode_ways)
        return mode, tm, tm * mode_ways + mode

    barrier = pltpu.get_barrier_semaphore()

    def greet(k, carry):
        mode, tm, _ = partner(k)
        pl.semaphore_signal(barrier, inc=1, device_id=(mode, tm), device_id_type=MESH)
        return carry

    lax.fori_loop(1, devices, greet, 0)
    loads = [
        pltpu.make_async_copy(src, dst, table_sems.at[5 + i])
        for i, (src, dst) in enumerate(
            ((x_hbm, x_ref), (table_hbm, table_ref), (twist_hbm, twist_ref))
        )
    ]
    for copy in loads:
        copy.start()

    def to_all(pick_src, dst, slot):
        def one(k, carry):
            mode, tm, holder = partner(k)
            pltpu.make_async_remote_copy(
                src_ref=pick_src(holder),
                dst_ref=dst,
                send_sem=send_sems.at[slot],
                recv_sem=recv_sems.at[slot],
                device_id=(mode, tm),
                device_id_type=MESH,
            ).start()
            return carry

        lax.fori_loop(1, devices, one, 0)

    def arrived(ref, slot):
        pltpu.make_async_copy(ref, ref, recv_sems.at[slot]).wait()

    def drained(ref, slot):
        pltpu.make_async_copy(ref, ref, send_sems.at[slot]).wait()

    def to_plane(g):
        pair = pl.ds(2 * g, 2)
        relay[:, :, my_mode, pair] = short[:, :, my_mode, pair]

        def one(k, carry):
            mode = lax.rem(my_mode + k, mode_ways)
            pltpu.make_async_remote_copy(
                src_ref=short.at[:, :, mode, pair],
                dst_ref=relay.at[:, :, my_mode, pair],
                send_sem=send_sems.at[slot_relay + g],
                recv_sem=recv_sems.at[slot_relay + g],
                device_id=(mode, my_tm),
                device_id_type=MESH,
            ).start()
            return carry

        lax.fori_loop(1, mode_ways, one, 0)

    def forward(i, slot):
        target = parts[1][1 + i][1].reshape(devices, planes, 4, half)
        mine = pl.ds(my_tm * mode_ways, mode_ways)

        def one(k, carry):
            tm = lax.rem(my_tm + k, tm_ways)
            pltpu.make_async_remote_copy(
                src_ref=relay.at[i, tm],
                dst_ref=target.at[mine],
                send_sem=send_sems.at[slot],
                recv_sem=recv_sems.at[slot],
                device_id=(my_mode, tm),
                device_id_type=MESH,
            ).start()
            return carry

        lax.fori_loop(1, tm_ways, one, 0)
        target[mine] = relay[i, my_tm]

    def spectral(load, step, base):
        m1, m2 = (m1h[...], m1l[...]), (m2h[...], m2l[...])

        def one(g, carry):
            if step == 0:
                make_rotor(g)
            real, imag = load(g)
            re, im = transform(real, imag, m1, m2, twist_ref, rotor_ref[0, g], rotor_ref[1, g])
            for part, value in enumerate((re, im)):
                for source, _, h, row, rows in parts[step]:
                    piece = value[:, h * half : (h + 1) * half].reshape(devices, 8, half)
                    source[:, 2 * g + part] = piece[:, row : row + rows]
            direct = parts[step] if step == 0 else parts[step][:1]
            for source, target, _, _, _ in direct:
                target[pl.ds(me * planes + 2 * g, 2)] = source[me, pl.ds(2 * g, 2)]
            if step == 1:
                to_plane(g)
            source, target = parts[step][0][:2]
            to_all(
                lambda holder: source.at[holder, pl.ds(2 * g, 2)],
                target.at[pl.ds(me * planes + 2 * g, 2)],
                base,
            )
            return carry

        lax.fori_loop(0, own, one, 0)
        if step == 1:
            for g in range(own):
                arrived(relay.at[:, :, pl.ds(0, mode_ways - 1), pl.ds(0, 2)], slot_relay + g)
            for i in range(2):
                forward(i, base + 1 + i)
            return
        source, target = parts[step][1][:2]
        to_all(
            lambda holder: source.at[holder], target.at[pl.ds(me * planes, planes)], base + 1
        )

    def order_quartets():
        quartet = quartets_ref[...]
        row = (quartet % modes_local // own * mode_ways + quartet // modes_local) * own
        row = row + quartet % own
        position = lax.broadcasted_iota(jnp.int32, (1, count), 1)
        lane = lax.broadcasted_iota(jnp.int32, (1, half), 1)
        spread = lambda line: jnp.broadcast_to(line, (half, count)).T
        key = row[0:1] * count + position
        places[4:5] = key
        spread_ref[4] = spread(key)
        for i in range(4):
            spread_ref[i] = spread(row[i : i + 1])
        weight_ref[...] = spread(intersections_ref[...])
        gather = lambda mask, values: jnp.sum(
            jnp.where(mask, values, jnp.zeros_like(values)), axis=0, keepdims=True
        )

        def rank_block(b, carry):
            here = pl.ds(pl.multiple_of(b * half, half), half)
            before = spread_ref[4] < places[4:5, here]
            places[5:6, here] = gather(before, jnp.ones((count, half), jnp.int32))
            return carry

        lax.fori_loop(0, count // half, rank_block, 0)
        spread_ref[4] = spread(places[5:6])

        def place_block(b, carry):
            here = pl.ds(pl.multiple_of(b * half, half), half)
            hit = spread_ref[4] == lane + b * half
            for i in range(4):
                places[i : i + 1, here] = gather(hit, spread_ref[i])
            shares[1:2, here] = gather(hit, weight_ref[...])
            return carry

        lax.fori_loop(0, count // half, place_block, 0)
        ones = jnp.ones((count, half), jnp.int32)
        below = gather(spread_ref[0] <= lane, ones)
        equal = gather(spread_ref[0] == lane, ones)
        places[4:5, :half] = jnp.maximum(below - 1, 0)
        shares[0:1, :half] = jnp.where(equal > 0, 1.0, 0.0)
        owner = places[0:1]
        same = jnp.logical_and(owner == pltpu.roll(owner, 1, 1), position > 0)
        keep_ref[...] = spread(jnp.where(same, 1.0, 0.0))
        weight_ref[...] = spread(shares[1:2])
        for i in range(1, 4):
            places[i : i + 1] = places[i : i + 1] * 2
        copies = [
            pltpu.make_async_copy(places.at[1 + i], ref, table_sems.at[i])
            for i, ref in enumerate((left_ref, middle_ref, right_ref))
        ]
        copies.append(
            pltpu.make_async_copy(places.at[4, pl.ds(0, half)], last_ref, table_sems.at[3])
        )
        copies.append(pltpu.make_async_copy(shares.at[0, pl.ds(0, half)], has_ref, table_sems.at[4]))
        for copy in copies:
            copy.start()
        for copy in copies:
            copy.wait()

    def evaluate(source, rows):
        load = lambda plane: (source[plane, :rows], source[plane + 1, :rows])

        def chunk(c, carry):
            acc_re, acc_im = carry
            for u in range(unroll):
                q = c * unroll + u
                re, im = triple_product(
                    load(left_ref[q]), load(middle_ref[q]), load(right_ref[q])
                )
                w = jnp.broadcast_to(weight_ref[pl.ds(q, 1), :], (rows, half))
                keep = jnp.broadcast_to(keep_ref[pl.ds(q, 1), :], (rows, half))
                acc_re = keep * acc_re - w * im
                acc_im = keep * acc_im + w * re
                partial[q, 0, :rows] = acc_re
                partial[q, 1, :rows] = acc_im
            return acc_re, acc_im

        zero = jnp.zeros((rows, half), jnp.float32)
        lax.fori_loop(0, count // unroll, chunk, (zero, zero))

    def kerr(step, part, store):
        _, source, _, _, rows = parts[step][part]
        evaluate(source, rows)

        def combine(d, carry):
            for g in range(own):
                row = d * own + g
                place, has = last_ref[row], has_ref[row]
                for r in range(2):
                    i = d * planes + 2 * g + r
                    value = has * partial[place, r, :rows]
                    first[i, :rows] = value
                    mid[i, :rows] = source[i] + value
            return carry

        lax.fori_loop(0, devices, combine, 0)
        evaluate(mid, rows)

        def finish(d, carry):
            for g in range(own):
                row = d * own + g
                place, has = last_ref[row], has_ref[row]
                squares = [0.0, 0.0]
                for r in range(2):
                    i = d * planes + 2 * g + r
                    second = has * partial[place, r, :rows]
                    new = source[i] + 0.5 * (first[i, :rows] + second)
                    estimate = 0.5 * (second - first[i, :rows])
                    store(d, 2 * g + r, new)
                    squares[0] += estimate * estimate
                    squares[1] += new * new
                for kind in range(2):
                    total = jnp.sum(squares[kind], axis=0, keepdims=True)
                    if part == 0:
                        sums[kind, pl.ds(row, 1)] = total
                    else:
                        sums[kind, pl.ds(row, 1)] += total
            return carry

        lax.fori_loop(0, devices, finish, 0)

    def fold(step):
        for kind in range(2):
            norm[pl.ds(2 * step + kind, 1)] = jnp.sum(sums[kind].T, axis=0, keepdims=True)

    norm[...] = jnp.zeros_like(norm)
    loads[0].wait()
    for g in range(own):
        for t in range(tm_ways):
            octet, line = divmod(t * own + g, 8)
            for r in range(2):
                for side in range(2):
                    rows = pl.ds(line + 8 * side, rows_local, stride=16)
                    staged[g, t, r, side] = x_ref[r, octet, rows, :]
        if g == 0:
            pl.semaphore_wait(barrier, devices - 1)
        columns[g, my_tm] = staged[g, my_tm]

        def fetch(k, carry, g=g):
            tm = lax.rem(my_tm + k, tm_ways)
            pltpu.make_async_remote_copy(
                src_ref=staged.at[g, tm],
                dst_ref=columns.at[g, my_tm],
                send_sem=send_sems.at[head + g],
                recv_sem=recv_sems.at[head + g],
                device_id=(my_mode, tm),
                device_id_type=MESH,
            ).start()
            return carry

        lax.fori_loop(1, tm_ways, fetch, 0)

    loads[1].wait()
    loads[2].wait()
    for part, (m1, m2) in enumerate(((m1h, m2h), (m1l, m2l))):
        re, im = table_ref[part, 0], table_ref[part, 1]
        for table, sign in ((m1, 1), (m2, -1)):
            table[:radix, :radix] = re
            table[radix:, radix:] = re
            table[:radix, radix:] = -im if sign == 1 else im
            table[radix:, :radix] = im if sign == 1 else -im

    order_quartets()

    def make_rotor(g):
        mode = my_tm * own + g
        offset, slope, curve = (beta_ref[i, mode] for i in range(3))
        offset, slope, curve = math.pi * offset, 300.0 * slope, 3000.0 * curve

        def strip(c, carry):
            start = pl.multiple_of(8 * c, 8)
            row = lax.broadcasted_iota(jnp.int32, (8, radix), 0) + start
            wave = row + radix * lax.broadcasted_iota(jnp.int32, (8, radix), 1)
            signed = jnp.where(wave < total_time // 2, wave, wave - total_time)
            frequency = signed.astype(jnp.float32) * (2.0 / total_time)
            phase = offset + slope * frequency + curve * frequency * frequency
            cosine, sine = cos_sin(phase)
            rotor_ref[0, g, pl.ds(start, 8)] = cosine * (1.0 / total_time)
            rotor_ref[1, g, pl.ds(start, 8)] = sine * (1.0 / total_time)
            return carry

        lax.fori_loop(0, radix // 8, strip, 0, unroll=4)

    def load_columns(g):
        arrived(columns.at[g, pl.ds(0, tm_ways - 1)], head + g)
        return [
            jnp.concatenate(
                [columns[g, :, r, side].reshape(radix, half) for side in range(2)], axis=1
            )
            for r in range(2)
        ]

    spectral(load_columns, 0, 0)

    def keep_update(h):
        def store(d, plane, value):
            updated[h, d, plane] = value

        return store

    arrived(held_00.at[pl.ds(0, (devices - 1) * planes)], 0)
    kerr(0, 0, keep_update(0))
    back[0, me] = updated[0, me]
    to_all(lambda holder: updated.at[0, holder], back.at[0, me], 2)
    arrived(held_01.at[pl.ds(0, (devices - 1) * planes)], 1)
    kerr(0, 1, keep_update(1))
    back[1, me] = updated[1, me]
    for g in range(own):
        to_all(
            lambda holder: updated.at[1, holder, pl.ds(2 * g, 2)],
            back.at[1, me, pl.ds(2 * g, 2)],
            3 + g,
        )
    fold(0)
    arrived(back.at[0, pl.ds(0, devices - 1)], 2)

    def load_back(g):
        arrived(back.at[1, pl.ds(0, devices - 1), pl.ds(0, 2)], 3 + g)
        pair = []
        for r in range(2):
            pair.append(
                jnp.concatenate(
                    [back[h, :, 2 * g + r].reshape(radix, half) for h in range(2)], axis=1
                )
            )
        return pair

    spectral(load_back, 1, slot_last)

    def last_update(h, row, count_rows):
        def store(d, plane, value):
            g, r = divmod(plane, 2)
            mode = d // mode_ways * own + g
            rows = pl.ds(lax.rem(mode, 8) + 8 * row, count_rows, stride=8)
            final.reshape(2, mode_ways, 2, octets, 64, half)[
                h, lax.rem(d, mode_ways), r, mode // 8, rows, :
            ] = value

        return store

    def home_part(i):
        _, _, h, row, rows = parts[1][i]
        lines = pl.ds(row, rows)
        return (lambda mode: final.at[h, mode, :, :, lines]), out_ref.at[:, :, my_mode, lines, h]

    def home_own(i):
        source, target = home_part(i)
        return pltpu.make_async_copy(source(my_mode), target, own_sems.at[i])

    def home(i):
        source, target = home_part(i)

        def one(k, carry):
            mode = lax.rem(my_mode + k, mode_ways)
            pltpu.make_async_remote_copy(
                src_ref=source(mode),
                dst_ref=target,
                send_sem=send_sems.at[slot_home + i],
                recv_sem=recv_sems.at[slot_home + i],
                device_id=(mode, my_tm),
                device_id_type=MESH,
            ).start()
            return carry

        lax.fori_loop(1, mode_ways, one, 0)
        home_own(i).start()

    def home_all(i):
        _, _, h, row, rows = parts[1][i]
        return final.at[h, pl.ds(0, mode_ways - 1), :, :, pl.ds(row, rows)]

    for i, (_, target, h, row, rows) in enumerate(parts[1]):
        sources = devices - 1 if i == 0 else devices - mode_ways
        arrived(target.at[pl.ds(0, sources * planes)], slot_last + i)
        kerr(1, i, last_update(h, row, rows))
        if i == len(parts[1]) - 1:
            fold(1)
            norms[me] = norm[...]
            to_all(lambda holder: norm, norms.at[me], slot_norm)
        home(i)
    arrived(norms.at[pl.ds(0, devices - 1)], slot_norm)
    total = jnp.sum(norms[...], axis=0)
    mode = lax.broadcasted_iota(jnp.int32, (devices * own, modes_local), 1)
    place = lax.broadcasted_iota(jnp.int32, (devices * own, modes_local), 0)
    pick = place == (mode // own * mode_ways + my_mode) * own + mode % own
    total = contract("ij,jk->ik", total, jnp.where(pick, 1.0, 0.0))
    err_ref[...] = jnp.concatenate(
        [
            jnp.sqrt(total[2 * s : 2 * s + 1] / (total[2 * s + 1 : 2 * s + 2] + epsilon))
            for s in range(STEPS)
        ],
        axis=0,
    )
    for i in range(len(parts[1])):
        arrived(home_all(i), slot_home + i)
        drained(home_all(i), slot_home + i)
        home_own(i).wait()
    for step, base in ((0, 0), (1, slot_last)):
        for i, (source, _, _, _, _) in enumerate(parts[step]):
            sources = devices - mode_ways if step == 1 and i > 0 else devices - 1
            drained(source.at[pl.ds(0, sources)], base + i)
    drained(updated.at[0, pl.ds(0, devices - 1)], slot_back)
    for g in range(own):
        drained(updated.at[1, pl.ds(0, devices - 1), pl.ds(0, 2)], slot_back + 1 + g)
        drained(columns.at[g, pl.ds(0, tm_ways - 1)], head + g)
        drained(relay.at[:, :, pl.ds(0, mode_ways - 1), pl.ds(0, 2)], slot_relay + g)
    drained(norms.at[pl.ds(0, devices - 1)], slot_norm)


def step_all(ways, own, beta, quartets, intersections, x, table, twist):
    mode_ways, tm_ways = ways
    devices = mode_ways * tm_ways
    planes = 2 * own
    count = quartets.shape[1]
    radix = twist.shape[1]
    half = radix // 2
    octets = x.shape[1]
    vmem = pl.BlockSpec(memory_space=pltpu.VMEM)
    smem = pl.BlockSpec(memory_space=pltpu.SMEM)
    real = lambda *shape: pltpu.VMEM(shape, jnp.float32)
    slots = 10 + 3 * own
    hbm = pl.BlockSpec(memory_space=pl.ANY)
    return pl.pallas_call(
        functools.partial(step_kernel, ways, own),
        in_specs=[smem, vmem, vmem, hbm, hbm, hbm],
        out_specs=[hbm, vmem],
        out_shape=[
            jax.ShapeDtypeStruct((2, octets, mode_ways, 8, 2, 8, half), jnp.float32),
            jax.ShapeDtypeStruct((STEPS, own * tm_ways), jnp.float32),
        ],
        scratch_shapes=[
            real(*x.shape),
            pltpu.VMEM(table.shape, table.dtype),
            real(*twist.shape),
            *[pltpu.VMEM((2 * radix, 2 * radix), jnp.bfloat16)] * 4,
            real(2, own, radix, radix),
            real(own, tm_ways, 2, 2, radix // tm_ways, half),
            real(own, tm_ways, 2, 2, radix // tm_ways, half),
            real(3, devices, planes, 8, half),
            *[real(2, tm_ways, mode_ways, planes, 4, half)] * 2,
            *[real(devices * planes, 8, half)] * 3,
            *[real(devices * planes, 4, half)] * 2,
            real(devices * planes, 8, half),
            real(devices * planes, 8, half),
            real(count, 2, 8, half),
            real(2, devices, planes, 8, half),
            real(2, devices, planes, 8, half),
            real(2, mode_ways, 2, octets, 8, 8, half),
            real(2, devices * own, half),
            real(8, devices * own),
            real(devices, 8, devices * own),
            pltpu.VMEM((8, count), jnp.int32),
            real(2, count),
            pltpu.VMEM((5, count, half), jnp.int32),
            real(count, half),
            real(count, half),
            *[pltpu.SMEM((count,), jnp.int32)] * 3,
            pltpu.SMEM((half,), jnp.int32),
            pltpu.SMEM((half,), jnp.float32),
            pltpu.SemaphoreType.DMA((slots,)),
            pltpu.SemaphoreType.DMA((slots,)),
            pltpu.SemaphoreType.DMA((8,)),
            pltpu.SemaphoreType.DMA((3,)),
        ],
        compiler_params=pltpu.CompilerParams(
            vmem_limit_bytes=56 * 1024 * 1024, collective_id=0, has_side_effects=True
        ),
        name="step_all",
    )(beta, quartets, intersections[None], x, table, twist)


def constant_tables(radix):
    position = np.arange(radix)
    product_of = position[:, None] * position[None, :]
    angle = -2.0 * np.pi / radix * (product_of % radix)
    table = np.stack([np.cos(angle), np.sin(angle)]).astype(np.float32)
    high = table.astype(jnp.bfloat16)
    low = (table - high.astype(np.float32)).astype(jnp.bfloat16)
    turn = -2.0 * np.pi / radix**2 * product_of
    twist = np.stack([np.cos(turn), np.sin(turn)]).astype(np.float32)
    return jnp.asarray(np.stack([high, low])), jnp.asarray(twist)


def shards(ways, field, beta, quartets, intersections):
    mode_ways, tm_ways = ways
    _, modes_local, time_local = field.shape
    radix = math.isqrt(time_local * tm_ways)
    own = modes_local // tm_ways
    table, twist = constant_tables(radix)
    octets, tiles = modes_local // 8, time_local // 128
    x = field.reshape(2, octets, 8, tiles, 128).transpose(0, 1, 3, 2, 4)
    x = x.reshape(2, octets, tiles * 8, 128)
    out, errors = step_all(ways, own, beta, quartets, intersections, x, table, twist)
    out = out.reshape(2, octets, tiles, 8, 128).transpose(0, 1, 3, 2, 4)
    return (out.reshape(2, modes_local, time_local), errors)


def solution(mesh):
    placed = (P(None, "mode", "tm"), P(None, "mode"), P(), P())

    def body(field, beta, quartets, intersections):
        mode_ways, tm_ways = mesh.shape["mode"], mesh.shape["tm"]
        devices = mode_ways * tm_ways
        total_time = field.shape[2] * tm_ways
        fits = field.shape[1] % tm_ways == 0 and RADIX == 8 * devices
        fits = fits and field.shape[1] % 8 == 0 and quartets.shape[1] % 128 == 0
        if fits and total_time == RADIX * RADIX and field.shape[1] * mode_ways == 128:
            return shards((mode_ways, tm_ways), field, beta, quartets, intersections)
        return shards_general(field, beta, quartets, intersections)

    return jax.shard_map(
        body,
        mesh=mesh,
        in_specs=placed,
        out_specs=(P(None, "mode", "tm"), P(None, "mode")),
        check_vma=False,
    )
```

```python
import functools
import math

import jax
import jax.numpy as jnp
import numpy as np
from jax import lax
from jax.experimental import pallas as pl
from jax.experimental.pallas import tpu as pltpu
from jax.sharding import PartitionSpec as P

RADIX = 256
STEPS = 2


epsilon = 1e-06


def phase_of(offset, slope, curve, frequency):
    return math.pi * offset + 300.0 * slope * frequency + 3000.0 * curve * frequency * frequency


def triple_product(left_field, middle_field, conj_field):
    prod_re = left_field[0] * middle_field[0] - left_field[1] * middle_field[1]
    prod_im = left_field[0] * middle_field[1] + left_field[1] * middle_field[0]
    out_re = prod_re * conj_field[0] + prod_im * conj_field[1]
    out_im = prod_im * conj_field[0] - prod_re * conj_field[1]
    return (out_re, out_im)


def contract(form, first_operand, second_operand):
    return jnp.einsum(form, first_operand, second_operand, precision=lax.Precision.HIGHEST)


def rotate(real_part, imag_part, angle):
    cosine = jnp.cos(angle)
    sine_part = jnp.sin(angle)
    return (real_part * cosine - imag_part * sine_part, real_part * sine_part + imag_part * cosine)


def dft_tables(length):
    positions = lax.iota(jnp.int32, length)
    product = positions[:, None] * positions[None, :] % length
    angle = -2.0 * math.pi / length * product.astype(jnp.float32)
    return (jnp.cos(angle), jnp.sin(angle))


def to_columns(state):
    return lax.all_to_all(state, "tm", split_axis=3, concat_axis=2, tiled=True)


def to_rows(state):
    return lax.all_to_all(state, "tm", split_axis=2, concat_axis=3, tiled=True)


def linear_step(state, beta, table_re, table_im):
    radix_size = table_re.shape[0]
    total_time = radix_size * radix_size
    cols_local = state.shape[3]
    tm_index = lax.axis_index("tm")
    head_re = contract("ka,mab->mkb", table_re, state[0]) - contract(
        "ka,mab->mkb", table_im, state[1]
    )
    head_im = contract("ka,mab->mkb", table_re, state[1]) + contract(
        "ka,mab->mkb", table_im, state[0]
    )
    column = tm_index * cols_local + lax.iota(jnp.int32, cols_local)
    row_position = lax.iota(jnp.int32, radix_size)
    twist = (
        -2.0
        * math.pi
        / total_time
        * (row_position[:, None] * column[None, :] % total_time).astype(jnp.float32)
    )
    head_re, head_im = rotate(head_re, head_im, twist[None])
    turned = lax.all_to_all(
        jnp.stack([head_re, head_im]), "tm", split_axis=2, concat_axis=3, tiled=True
    )
    spec_re = contract("mcb,kb->mck", turned[0], table_re) - contract(
        "mcb,kb->mck", turned[1], table_im
    )
    spec_im = contract("mcb,kb->mck", turned[1], table_re) + contract(
        "mcb,kb->mck", turned[0], table_im
    )
    rows_local = turned.shape[2]
    first_index = tm_index * rows_local + lax.iota(jnp.int32, rows_local)
    wave = first_index[:, None] + radix_size * row_position[None, :]
    signed = jnp.where(wave < total_time // 2, wave, wave - total_time)
    frequency = signed.astype(jnp.float32) / (total_time / 2)
    angle = phase_of(
        beta[0][:, None, None], beta[1][:, None, None], beta[2][:, None, None], frequency[None]
    )
    spec_re, spec_im = rotate(spec_re, spec_im, angle)
    back_re = contract("mck,kb->mcb", spec_re, table_re) + contract(
        "mck,kb->mcb", spec_im, table_im
    )
    back_im = contract("mck,kb->mcb", spec_im, table_re) - contract(
        "mck,kb->mcb", spec_re, table_im
    )
    untwist = (
        2.0
        * math.pi
        / total_time
        * (first_index[:, None] * row_position[None, :] % total_time).astype(jnp.float32)
    )
    back_re, back_im = rotate(back_re, back_im, untwist[None])
    gathered = lax.all_to_all(
        jnp.stack([back_re, back_im]), "tm", split_axis=3, concat_axis=2, tiled=True
    )
    scale = 1.0 / total_time
    out_re = (
        contract("ka,mkb->mab", table_re, gathered[0])
        + contract("ka,mkb->mab", table_im, gathered[1])
    ) * scale
    out_im = (
        contract("ka,mkb->mab", table_re, gathered[1])
        - contract("ka,mkb->mab", table_im, gathered[0])
    ) * scale
    return jnp.stack([out_re, out_im])


def kerr_term(fields, quartets, intersections):
    count = quartets.shape[1]
    block_size = min(512, count)
    blocks = count // block_size
    grouped = quartets.reshape(4, blocks, block_size).transpose(1, 0, 2)
    weights = intersections.reshape(blocks, block_size)
    modes_all = fields.shape[1]
    mode_ids = lax.iota(jnp.int32, modes_all)

    def accumulate(running, block_item):
        indices, weight = block_item
        out_re, out_im = triple_product(
            jnp.take(fields, indices[1], axis=1),
            jnp.take(fields, indices[2], axis=1),
            jnp.take(fields, indices[3], axis=1),
        )
        owner = (indices[0][None, :] == mode_ids[:, None]).astype(jnp.float32) * weight[None, :]
        add_re = contract("pq,qt->pt", owner, -out_im)
        add_im = contract("pq,qt->pt", owner, out_re)
        return (running + jnp.stack([add_re, add_im]), None)

    running, unused = lax.scan(accumulate, jnp.zeros_like(fields), (grouped, weights))
    return running


def kerr_step(flat, quartets, intersections):
    spread = lax.all_to_all(flat, "mode", split_axis=2, concat_axis=1, tiled=True)
    first = kerr_term(spread, quartets, intersections)
    second = kerr_term(spread + first, quartets, intersections)
    updated = spread + 0.5 * (first + second)
    estimate = 0.5 * (second - first)
    returned, estimate_home = (
        lax.all_to_all(updated, "mode", split_axis=1, concat_axis=2, tiled=True),
        lax.all_to_all(estimate, "mode", split_axis=1, concat_axis=2, tiled=True),
    )
    error_part = jnp.sum(estimate_home * estimate_home, axis=(0, 2))
    field_part = jnp.sum(returned * returned, axis=(0, 2))
    return (returned, error_part, field_part)


def shards_general(field, beta, quartets, intersections):
    modes_local = field.shape[1]
    time_local = field.shape[2]
    table_re, table_im = dft_tables(RADIX)
    state = field.reshape(2, modes_local, time_local // RADIX, RADIX)
    state = to_columns(state)
    error_rows = []
    for step_index in range(STEPS):
        columns = state
        columns = linear_step(columns, beta, table_re, table_im)
        updated, error_part, field_part = kerr_step(
            columns.reshape(2, modes_local, time_local), quartets, intersections
        )
        error_sq, field_sq = lax.psum((error_part, field_part), "tm")
        error_rows.append(jnp.sqrt(error_sq / (field_sq + epsilon)))
        state = updated.reshape(columns.shape)
    state = to_rows(state)
    errors = jnp.stack(error_rows)
    return (state.reshape(2, modes_local, time_local), errors)


UNROLL = 32
MESH = pl.DeviceIdType.MESH


def half_pi_terms():
    whole = math.pi / 2
    first = math.floor(whole * 2**11) / 2**11
    second = math.floor((whole - first) * 2**23) / 2**23
    return first, second, whole - first - second


HALF_PI = half_pi_terms()


def split(value):
    high = value.astype(jnp.bfloat16)
    low = (value - high.astype(jnp.float32)).astype(jnp.bfloat16)
    return high, low


def split_table(value):
    high = lax.reduce_precision(value, exponent_bits=8, mantissa_bits=7)
    return high.astype(jnp.bfloat16), (value - high).astype(jnp.bfloat16)


def product(left, right):
    dot = lambda a, b: jnp.dot(a, b, preferred_element_type=jnp.float32)
    return dot(left[0], right[0]) + (dot(left[0], right[1]) + dot(left[1], right[0]))


def transform(real, imag, m1, m2, twist_ref, ro_re, ro_im):
    radix = twist_ref.shape[1]
    head = product(m1, split(jnp.concatenate([real, imag], axis=0)))
    head_re, head_im = head[:radix], head[radix:]
    tw_re, tw_im = twist_ref[0], twist_ref[1]
    re = head_re * tw_re - head_im * tw_im
    im = head_re * tw_im + head_im * tw_re
    spec = product(split(jnp.concatenate([re, im], axis=1)), m2)
    spec_re, spec_im = spec[:, :radix], spec[:, radix:]
    re = spec_re * ro_re - spec_im * ro_im
    im = spec_re * ro_im + spec_im * ro_re
    back = product(split(jnp.concatenate([re, im], axis=1)), m1)
    back_re, back_im = back[:, :radix], back[:, radix:]
    re = back_re * tw_re + back_im * tw_im
    im = back_im * tw_re - back_re * tw_im
    out = product(m2, split(jnp.concatenate([re, im], axis=0)))
    return out[:radix], out[radix:]


def cos_sin(angle):
    turns = jnp.round(angle * (2.0 / math.pi))
    rest = angle - turns * HALF_PI[0]
    rest = rest - turns * HALF_PI[1]
    rest = rest - turns * HALF_PI[2]
    square = rest * rest
    sine = -1.9515295891e-4 * square + 8.3321608736e-3
    sine = (sine * square - 1.6666654611e-1) * square * rest + rest
    cosine = 2.443315711809948e-5 * square - 1.388731625493765e-3
    cosine = (cosine * square + 4.166664568298827e-2) * square * square - 0.5 * square + 1.0
    quarter = turns.astype(jnp.int32)
    odd = (quarter & 1) == 1
    cos_part = jnp.where(odd, sine, cosine)
    sin_part = jnp.where(odd, cosine, sine)
    cos_part = jnp.where(((quarter + 1) & 2) == 2, -cos_part, cos_part)
    sin_part = jnp.where((quarter & 2) == 2, -sin_part, sin_part)
    return cos_part, sin_part


def step_kernel(
    ways, own, beta_hbm, quartets_hbm, intersections_hbm, x_hbm, table_hbm, twist_hbm,
    out_ref, err_out,
    beta_ref, quartets_ref, intersections_ref, err_ref, x_ref, table_ref, twist_ref,
    m1h, m1l, m2h, m2l, rotor_ref, staged, columns,
    sent, short, relay, held_00, held_01, held_10, held_11, held_12, mid, first, partial, updated, back, final, sums, norm, norms,
    places, shares, spread_ref, weight_ref, keep_ref, left_ref, middle_ref, right_ref, last_ref, has_ref,
    send_sems, recv_sems, table_sems, own_sems,
):
    mode_ways, tm_ways = ways
    devices = mode_ways * tm_ways
    planes = 2 * own
    my_mode, my_tm = lax.axis_index("mode"), lax.axis_index("tm")
    me = my_tm * mode_ways + my_mode
    radix = twist_ref.shape[1]
    half = radix // 2
    parts = (
        ((sent.at[0], held_00, 0, 0, 8), (sent.at[1], held_01, 1, 0, 8)),
        (
            (sent.at[2], held_10, 0, 0, 8),
            (short.at[0].reshape(devices, planes, 4, half), held_11, 1, 0, 4),
            (short.at[1].reshape(devices, planes, 4, half), held_12, 1, 4, 4),
        ),
    )
    count = weight_ref.shape[0]
    modes_local = own * tm_ways
    unroll = UNROLL if count % UNROLL == 0 else 1
    total_time = radix * radix
    rows_local = radix // tm_ways
    slot_back, slot_last = 2, 3 + own
    slot_home, slot_norm, head = slot_last + 3, slot_last + 6, slot_last + 7
    slot_relay = head + own
    octets = x_ref.shape[1]

    def partner(k):
        tm = lax.rem(my_tm + lax.rem(k, tm_ways), tm_ways)
        mode = lax.rem(my_mode + k // tm_ways, mode_ways)
        return mode, tm, tm * mode_ways + mode

    barrier = pltpu.get_barrier_semaphore()

    def greet(k, carry):
        mode, tm, _ = partner(k)
        pl.semaphore_signal(barrier, inc=1, device_id=(mode, tm), device_id_type=MESH)
        return carry

    lax.fori_loop(1, devices, greet, 0)
    loads = [
        pltpu.make_async_copy(src, dst, table_sems.at[5 + i])
        for i, (src, dst) in enumerate(
            (
                (x_hbm, x_ref),
                (table_hbm, table_ref),
                (twist_hbm, twist_ref),
                (beta_hbm, beta_ref),
                (quartets_hbm, quartets_ref),
                (intersections_hbm, intersections_ref),
            )
        )
    ]
    for copy in loads:
        copy.start()

    def to_all(pick_src, dst, slot):
        def one(k, carry):
            mode, tm, holder = partner(k)
            pltpu.make_async_remote_copy(
                src_ref=pick_src(holder),
                dst_ref=dst,
                send_sem=send_sems.at[slot],
                recv_sem=recv_sems.at[slot],
                device_id=(mode, tm),
                device_id_type=MESH,
            ).start()
            return carry

        lax.fori_loop(1, devices, one, 0)

    def arrived(ref, slot):
        pltpu.make_async_copy(ref, ref, recv_sems.at[slot]).wait()

    def drained(ref, slot):
        pltpu.make_async_copy(ref, ref, send_sems.at[slot]).wait()

    def to_plane(g):
        pair = pl.ds(2 * g, 2)
        relay[:, :, my_mode, pair] = short[:, :, my_mode, pair]

        def one(k, carry):
            mode = lax.rem(my_mode + k, mode_ways)
            pltpu.make_async_remote_copy(
                src_ref=short.at[:, :, mode, pair],
                dst_ref=relay.at[:, :, my_mode, pair],
                send_sem=send_sems.at[slot_relay + g],
                recv_sem=recv_sems.at[slot_relay + g],
                device_id=(mode, my_tm),
                device_id_type=MESH,
            ).start()
            return carry

        lax.fori_loop(1, mode_ways, one, 0)

    def forward(i, slot):
        target = parts[1][1 + i][1].reshape(devices, planes, 4, half)
        mine = pl.ds(my_tm * mode_ways, mode_ways)

        def one(k, carry):
            tm = lax.rem(my_tm + k, tm_ways)
            pltpu.make_async_remote_copy(
                src_ref=relay.at[i, tm],
                dst_ref=target.at[mine],
                send_sem=send_sems.at[slot],
                recv_sem=recv_sems.at[slot],
                device_id=(my_mode, tm),
                device_id_type=MESH,
            ).start()
            return carry

        lax.fori_loop(1, tm_ways, one, 0)
        target[mine] = relay[i, my_tm]

    def spectral(load, step, base):
        m1, m2 = (m1h[...], m1l[...]), (m2h[...], m2l[...])

        def one(g, carry):
            if step == 0:
                make_rotor(g)
            real, imag = load(g)
            re, im = transform(real, imag, m1, m2, twist_ref, rotor_ref[0, g], rotor_ref[1, g])
            for part, value in enumerate((re, im)):
                for source, _, h, row, rows in parts[step]:
                    piece = value[:, h * half : (h + 1) * half].reshape(devices, 8, half)
                    source[:, 2 * g + part] = piece[:, row : row + rows]
            direct = parts[step] if step == 0 else parts[step][:1]
            for source, target, _, _, _ in direct:
                target[pl.ds(me * planes + 2 * g, 2)] = source[me, pl.ds(2 * g, 2)]
            if step == 1:
                to_plane(g)
            source, target = parts[step][0][:2]
            to_all(
                lambda holder: source.at[holder, pl.ds(2 * g, 2)],
                target.at[pl.ds(me * planes + 2 * g, 2)],
                base,
            )
            return carry

        lax.fori_loop(0, own, one, 0)
        if step == 1:
            for g in range(own):
                arrived(relay.at[:, :, pl.ds(0, mode_ways - 1), pl.ds(0, 2)], slot_relay + g)
            for i in range(2):
                forward(i, base + 1 + i)
            return
        source, target = parts[step][1][:2]
        to_all(
            lambda holder: source.at[holder], target.at[pl.ds(me * planes, planes)], base + 1
        )

    def order_quartets():
        quartet = quartets_ref[...]
        row = (quartet % modes_local // own * mode_ways + quartet // modes_local) * own
        row = row + quartet % own
        position = lax.broadcasted_iota(jnp.int32, (1, count), 1)
        lane = lax.broadcasted_iota(jnp.int32, (1, half), 1)
        spread = lambda line: jnp.broadcast_to(line, (half, count)).T
        key = row[0:1] * count + position
        places[4:5] = key
        spread_ref[4] = spread(key)
        for i in range(4):
            spread_ref[i] = spread(row[i : i + 1])
        weight_ref[...] = spread(intersections_ref[...])
        gather = lambda mask, values: jnp.sum(
            jnp.where(mask, values, jnp.zeros_like(values)), axis=0, keepdims=True
        )

        def rank_block(b, carry):
            here = pl.ds(pl.multiple_of(b * half, half), half)
            before = spread_ref[4] < places[4:5, here]
            places[5:6, here] = gather(before, jnp.ones((count, half), jnp.int32))
            return carry

        lax.fori_loop(0, count // half, rank_block, 0)
        spread_ref[4] = spread(places[5:6])

        def place_block(b, carry):
            here = pl.ds(pl.multiple_of(b * half, half), half)
            hit = spread_ref[4] == lane + b * half
            for i in range(4):
                places[i : i + 1, here] = gather(hit, spread_ref[i])
            shares[1:2, here] = gather(hit, weight_ref[...])
            return carry

        lax.fori_loop(0, count // half, place_block, 0)
        ones = jnp.ones((count, half), jnp.int32)
        below = gather(spread_ref[0] <= lane, ones)
        equal = gather(spread_ref[0] == lane, ones)
        places[4:5, :half] = jnp.maximum(below - 1, 0)
        shares[0:1, :half] = jnp.where(equal > 0, 1.0, 0.0)
        owner = places[0:1]
        same = jnp.logical_and(owner == pltpu.roll(owner, 1, 1), position > 0)
        keep_ref[...] = spread(jnp.where(same, 1.0, 0.0))
        weight_ref[...] = spread(shares[1:2])
        for i in range(1, 4):
            places[i : i + 1] = places[i : i + 1] * 2
        copies = [
            pltpu.make_async_copy(places.at[1 + i], ref, table_sems.at[i])
            for i, ref in enumerate((left_ref, middle_ref, right_ref))
        ]
        copies.append(
            pltpu.make_async_copy(places.at[4, pl.ds(0, half)], last_ref, table_sems.at[3])
        )
        copies.append(pltpu.make_async_copy(shares.at[0, pl.ds(0, half)], has_ref, table_sems.at[4]))
        for copy in copies:
            copy.start()
        for copy in copies:
            copy.wait()

    def evaluate(source, rows):
        load = lambda plane: (source[plane, :rows], source[plane + 1, :rows])

        def chunk(c, carry):
            acc_re, acc_im = carry
            for u in range(unroll):
                q = c * unroll + u
                re, im = triple_product(
                    load(left_ref[q]), load(middle_ref[q]), load(right_ref[q])
                )
                w = jnp.broadcast_to(weight_ref[pl.ds(q, 1), :], (rows, half))
                keep = jnp.broadcast_to(keep_ref[pl.ds(q, 1), :], (rows, half))
                acc_re = keep * acc_re - w * im
                acc_im = keep * acc_im + w * re
                partial[q, 0, :rows] = acc_re
                partial[q, 1, :rows] = acc_im
            return acc_re, acc_im

        zero = jnp.zeros((rows, half), jnp.float32)
        lax.fori_loop(0, count // unroll, chunk, (zero, zero))

    def kerr(step, part, store):
        _, source, _, _, rows = parts[step][part]
        evaluate(source, rows)

        def combine(d, carry):
            for g in range(own):
                row = d * own + g
                place, has = last_ref[row], has_ref[row]
                for r in range(2):
                    i = d * planes + 2 * g + r
                    value = has * partial[place, r, :rows]
                    first[i, :rows] = value
                    mid[i, :rows] = source[i] + value
            return carry

        lax.fori_loop(0, devices, combine, 0, unroll=2)
        evaluate(mid, rows)

        def finish(d, carry):
            for g in range(own):
                row = d * own + g
                place, has = last_ref[row], has_ref[row]
                squares = [0.0, 0.0]
                for r in range(2):
                    i = d * planes + 2 * g + r
                    second = has * partial[place, r, :rows]
                    new = source[i] + 0.5 * (first[i, :rows] + second)
                    estimate = 0.5 * (second - first[i, :rows])
                    store(d, 2 * g + r, new)
                    squares[0] += estimate * estimate
                    squares[1] += new * new
                for kind in range(2):
                    total = jnp.sum(squares[kind], axis=0, keepdims=True)
                    if part == 0:
                        sums[kind, pl.ds(row, 1)] = total
                    else:
                        sums[kind, pl.ds(row, 1)] += total
            return carry

        lax.fori_loop(0, devices, finish, 0, unroll=2)

    def fold(step):
        for kind in range(2):
            norm[pl.ds(2 * step + kind, 1)] = jnp.sum(sums[kind].T, axis=0, keepdims=True)

    norm[...] = jnp.zeros_like(norm)
    loads[0].wait()
    for g in range(own):
        for t in range(tm_ways):
            octet, line = divmod(t * own + g, 8)
            for r in range(2):
                for side in range(2):
                    rows = pl.ds(line + 8 * side, rows_local, stride=16)
                    staged[g, t, r, side] = x_ref[r, octet, rows, :]
        if g == 0:
            pl.semaphore_wait(barrier, devices - 1)
        columns[g, my_tm] = staged[g, my_tm]

        def fetch(k, carry, g=g):
            tm = lax.rem(my_tm + k, tm_ways)
            pltpu.make_async_remote_copy(
                src_ref=staged.at[g, tm],
                dst_ref=columns.at[g, my_tm],
                send_sem=send_sems.at[head + g],
                recv_sem=recv_sems.at[head + g],
                device_id=(my_mode, tm),
                device_id_type=MESH,
            ).start()
            return carry

        lax.fori_loop(1, tm_ways, fetch, 0)

    for copy in loads[1:]:
        copy.wait()
    for part, (m1, m2) in enumerate(((m1h, m2h), (m1l, m2l))):
        re, im = table_ref[part, 0], table_ref[part, 1]
        for table, sign in ((m1, 1), (m2, -1)):
            table[:radix, :radix] = re
            table[radix:, radix:] = re
            table[:radix, radix:] = -im if sign == 1 else im
            table[radix:, :radix] = im if sign == 1 else -im

    order_quartets()

    def make_rotor(g):
        mode = my_tm * own + g
        offset, slope, curve = (beta_ref[i, mode] for i in range(3))
        offset, slope, curve = math.pi * offset, 300.0 * slope, 3000.0 * curve

        def strip(c, carry):
            start = pl.multiple_of(8 * c, 8)
            row = lax.broadcasted_iota(jnp.int32, (8, radix), 0) + start
            wave = row + radix * lax.broadcasted_iota(jnp.int32, (8, radix), 1)
            signed = jnp.where(wave < total_time // 2, wave, wave - total_time)
            frequency = signed.astype(jnp.float32) * (2.0 / total_time)
            phase = offset + slope * frequency + curve * frequency * frequency
            cosine, sine = cos_sin(phase)
            rotor_ref[0, g, pl.ds(start, 8)] = cosine * (1.0 / total_time)
            rotor_ref[1, g, pl.ds(start, 8)] = sine * (1.0 / total_time)
            return carry

        lax.fori_loop(0, radix // 8, strip, 0, unroll=4)

    def load_columns(g):
        arrived(columns.at[g, pl.ds(0, tm_ways - 1)], head + g)
        return [
            jnp.concatenate(
                [columns[g, :, r, side].reshape(radix, half) for side in range(2)], axis=1
            )
            for r in range(2)
        ]

    spectral(load_columns, 0, 0)

    def keep_update(h):
        def store(d, plane, value):
            updated[h, d, plane] = value

        return store

    arrived(held_00.at[pl.ds(0, (devices - 1) * planes)], 0)
    kerr(0, 0, keep_update(0))
    back[0, me] = updated[0, me]
    to_all(lambda holder: updated.at[0, holder], back.at[0, me], 2)
    arrived(held_01.at[pl.ds(0, (devices - 1) * planes)], 1)
    kerr(0, 1, keep_update(1))
    back[1, me] = updated[1, me]
    for g in range(own):
        to_all(
            lambda holder: updated.at[1, holder, pl.ds(2 * g, 2)],
            back.at[1, me, pl.ds(2 * g, 2)],
            3 + g,
        )
    fold(0)
    arrived(back.at[0, pl.ds(0, devices - 1)], 2)

    def load_back(g):
        arrived(back.at[1, pl.ds(0, devices - 1), pl.ds(0, 2)], 3 + g)
        pair = []
        for r in range(2):
            pair.append(
                jnp.concatenate(
                    [back[h, :, 2 * g + r].reshape(radix, half) for h in range(2)], axis=1
                )
            )
        return pair

    spectral(load_back, 1, slot_last)

    def last_update(h, row, count_rows):
        def store(d, plane, value):
            g, r = divmod(plane, 2)
            mode = d // mode_ways * own + g
            rows = pl.ds(lax.rem(mode, 8) + 8 * row, count_rows, stride=8)
            final.reshape(2, mode_ways, 2, octets, 64, half)[
                h, lax.rem(d, mode_ways), r, mode // 8, rows, :
            ] = value

        return store

    def home_part(i):
        _, _, h, row, rows = parts[1][i]
        lines = pl.ds(row, rows)
        return (lambda mode: final.at[h, mode, :, :, lines]), out_ref.at[:, :, my_mode, lines, h]

    def home_own(i):
        source, target = home_part(i)
        return pltpu.make_async_copy(source(my_mode), target, own_sems.at[i])

    def home(i):
        source, target = home_part(i)

        def one(k, carry):
            mode = lax.rem(my_mode + k, mode_ways)
            pltpu.make_async_remote_copy(
                src_ref=source(mode),
                dst_ref=target,
                send_sem=send_sems.at[slot_home + i],
                recv_sem=recv_sems.at[slot_home + i],
                device_id=(mode, my_tm),
                device_id_type=MESH,
            ).start()
            return carry

        lax.fori_loop(1, mode_ways, one, 0)
        home_own(i).start()

    def home_all(i):
        _, _, h, row, rows = parts[1][i]
        return final.at[h, pl.ds(0, mode_ways - 1), :, :, pl.ds(row, rows)]

    for i, (_, target, h, row, rows) in enumerate(parts[1]):
        sources = devices - 1 if i == 0 else devices - mode_ways
        arrived(target.at[pl.ds(0, sources * planes)], slot_last + i)
        kerr(1, i, last_update(h, row, rows))
        if i == len(parts[1]) - 1:
            fold(1)
            norms[me] = norm[...]
            to_all(lambda holder: norm, norms.at[me], slot_norm)
        home(i)
    arrived(norms.at[pl.ds(0, devices - 1)], slot_norm)
    total = jnp.sum(norms[...], axis=0)
    mode = lax.broadcasted_iota(jnp.int32, (devices * own, modes_local), 1)
    place = lax.broadcasted_iota(jnp.int32, (devices * own, modes_local), 0)
    pick = place == (mode // own * mode_ways + my_mode) * own + mode % own
    total = contract("ij,jk->ik", total, jnp.where(pick, 1.0, 0.0))
    err_ref[...] = jnp.concatenate(
        [
            jnp.sqrt(total[2 * s : 2 * s + 1] / (total[2 * s + 1 : 2 * s + 2] + epsilon))
            for s in range(STEPS)
        ],
        axis=0,
    )
    err_copy = pltpu.make_async_copy(err_ref, err_out, table_sems.at[11])
    err_copy.start()
    for i in range(len(parts[1])):
        arrived(home_all(i), slot_home + i)
        drained(home_all(i), slot_home + i)
        home_own(i).wait()
    for step, base in ((0, 0), (1, slot_last)):
        for i, (source, _, _, _, _) in enumerate(parts[step]):
            sources = devices - mode_ways if step == 1 and i > 0 else devices - 1
            drained(source.at[pl.ds(0, sources)], base + i)
    drained(updated.at[0, pl.ds(0, devices - 1)], slot_back)
    for g in range(own):
        drained(updated.at[1, pl.ds(0, devices - 1), pl.ds(0, 2)], slot_back + 1 + g)
        drained(columns.at[g, pl.ds(0, tm_ways - 1)], head + g)
        drained(relay.at[:, :, pl.ds(0, mode_ways - 1), pl.ds(0, 2)], slot_relay + g)
    drained(norms.at[pl.ds(0, devices - 1)], slot_norm)
    err_copy.wait()


def step_all(ways, own, beta, quartets, intersections, x, table, twist):
    mode_ways, tm_ways = ways
    devices = mode_ways * tm_ways
    planes = 2 * own
    count = quartets.shape[1]
    radix = twist.shape[1]
    half = radix // 2
    octets = x.shape[1]
    real = lambda *shape: pltpu.VMEM(shape, jnp.float32)
    slots = 10 + 3 * own
    hbm = pl.BlockSpec(memory_space=pl.ANY)
    return pl.pallas_call(
        functools.partial(step_kernel, ways, own),
        in_specs=[hbm] * 6,
        out_specs=[pl.BlockSpec(memory_space=pltpu.VMEM)] * 2,
        out_shape=[
            pltpu.VMEM((2, octets, mode_ways, 8, 2, 8, half), jnp.float32),
            pltpu.VMEM((STEPS, own * tm_ways), jnp.float32),
        ],
        scratch_shapes=[
            pltpu.SMEM(beta.shape, beta.dtype),
            pltpu.VMEM(quartets.shape, quartets.dtype),
            real(1, count),
            real(STEPS, own * tm_ways),
            real(*x.shape),
            pltpu.VMEM(table.shape, table.dtype),
            real(*twist.shape),
            *[pltpu.VMEM((2 * radix, 2 * radix), jnp.bfloat16)] * 4,
            real(2, own, radix, radix),
            real(own, tm_ways, 2, 2, radix // tm_ways, half),
            real(own, tm_ways, 2, 2, radix // tm_ways, half),
            real(3, devices, planes, 8, half),
            *[real(2, tm_ways, mode_ways, planes, 4, half)] * 2,
            *[real(devices * planes, 8, half)] * 3,
            *[real(devices * planes, 4, half)] * 2,
            real(devices * planes, 8, half),
            real(devices * planes, 8, half),
            real(count, 2, 8, half),
            real(2, devices, planes, 8, half),
            real(2, devices, planes, 8, half),
            real(2, mode_ways, 2, octets, 8, 8, half),
            real(2, devices * own, half),
            real(8, devices * own),
            real(devices, 8, devices * own),
            pltpu.VMEM((8, count), jnp.int32),
            real(2, count),
            pltpu.VMEM((5, count, half), jnp.int32),
            real(count, half),
            real(count, half),
            *[pltpu.SMEM((count,), jnp.int32)] * 3,
            pltpu.SMEM((half,), jnp.int32),
            pltpu.SMEM((half,), jnp.float32),
            pltpu.SemaphoreType.DMA((slots,)),
            pltpu.SemaphoreType.DMA((slots,)),
            pltpu.SemaphoreType.DMA((12,)),
            pltpu.SemaphoreType.DMA((3,)),
        ],
        compiler_params=pltpu.CompilerParams(
            vmem_limit_bytes=52 * 1024 * 1024, collective_id=0, has_side_effects=True
        ),
        name="step_all",
    )(beta, quartets, intersections[None], x, table, twist)


def emit_kernel(out_ref, err_ref, out_hbm, err_hbm, sems):
    copies = [
        pltpu.make_async_copy(out_ref, out_hbm, sems.at[0]),
        pltpu.make_async_copy(err_ref, err_hbm, sems.at[1]),
    ]
    for copy in copies:
        copy.start()
    for copy in copies:
        copy.wait()


def emit(out, errors):
    return pl.pallas_call(
        emit_kernel,
        in_specs=[pl.BlockSpec(memory_space=pltpu.VMEM)] * 2,
        out_specs=[pl.BlockSpec(memory_space=pl.ANY)] * 2,
        out_shape=[jax.ShapeDtypeStruct(a.shape, jnp.float32) for a in (out, errors)],
        scratch_shapes=[pltpu.SemaphoreType.DMA((2,))],
        compiler_params=pltpu.CompilerParams(vmem_limit_bytes=1024 * 1024),
        name="emit",
    )(out, errors)


def constant_tables(radix):
    position = np.arange(radix)
    product_of = position[:, None] * position[None, :]
    angle = -2.0 * np.pi / radix * (product_of % radix)
    table = np.stack([np.cos(angle), np.sin(angle)]).astype(np.float32)
    high = table.astype(jnp.bfloat16)
    low = (table - high.astype(np.float32)).astype(jnp.bfloat16)
    turn = -2.0 * np.pi / radix**2 * product_of
    twist = np.stack([np.cos(turn), np.sin(turn)]).astype(np.float32)
    return jnp.asarray(np.stack([high, low])), jnp.asarray(twist)


def shards(ways, field, beta, quartets, intersections):
    mode_ways, tm_ways = ways
    _, modes_local, time_local = field.shape
    radix = math.isqrt(time_local * tm_ways)
    own = modes_local // tm_ways
    table, twist = constant_tables(radix)
    octets, tiles = modes_local // 8, time_local // 128
    x = field.reshape(2, octets, 8, tiles, 128).transpose(0, 1, 3, 2, 4)
    x = x.reshape(2, octets, tiles * 8, 128)
    out, errors = emit(*step_all(ways, own, beta, quartets, intersections, x, table, twist))
    out = out.reshape(2, octets, tiles, 8, 128).transpose(0, 1, 3, 2, 4)
    return (out.reshape(2, modes_local, time_local), errors)


def solution(mesh):
    placed = (P(None, "mode", "tm"), P(None, "mode"), P(), P())

    def body(field, beta, quartets, intersections):
        mode_ways, tm_ways = mesh.shape["mode"], mesh.shape["tm"]
        devices = mode_ways * tm_ways
        total_time = field.shape[2] * tm_ways
        fits = field.shape[1] % tm_ways == 0 and RADIX == 8 * devices
        fits = fits and field.shape[1] % 8 == 0 and quartets.shape[1] % 128 == 0
        if fits and total_time == RADIX * RADIX and field.shape[1] * mode_ways == 128:
            return shards((mode_ways, tm_ways), field, beta, quartets, intersections)
        return shards_general(field, beta, quartets, intersections)

    return jax.shard_map(
        body,
        mesh=mesh,
        in_specs=placed,
        out_specs=(P(None, "mode", "tm"), P(None, "mode")),
        check_vma=False,
    )
```
